32 devices in a mesh: rep: 4 (over y, x), tp: 8 (over z, core).
Axes of the slice: x: 2, y: 2, z: 4, core: 2. Of those that a mesh axis runs over, the one named last changes fastest.
Arguments:
- residual: bfloat16 [4, 1024, 4096], P('rep', 'tp'), may hold values from -6 to 6
- gate_pre: bfloat16 [4, 1024, 7168], P('rep', None, 'tp'), may hold values from -6 to 6
- up_pre: bfloat16 [4, 1024, 7168], P('rep', None, 'tp'), may hold values from -6 to 6
- down_weight: bfloat16 [7168, 4096], P('tp'), may hold values from -0.0625 to 0.0625
- d_out: bfloat16 [4, 1024, 4096], P('rep', 'tp'), may hold values from -1.5 to 1.5
- comp_index: int32 [4, 112, 2048], P('rep', 'tp'), may hold values from 0 to 4095
- comp_value: bfloat16 [4, 112, 2048], P('rep', 'tp'), may hold values from -48 to 48
Outputs:
- output: bfloat16 [4, 1024, 4096], P('rep', 'tp')
- gate_preact_gradient: bfloat16 [4, 1024, 7168], P('rep', None, 'tp')
- up_grad: bfloat16 [4, 1024, 7168], P('rep', None, 'tp')
- weight_grad: bfloat16 [4, 7168, 4096], P('rep', 'tp')
- update: bfloat16 [7168, 4096], P('tp')
- updated_down_weight: bfloat16 [7168, 4096], P('tp')
The draws below stay inside these ranges and needn't reach their ends.
Inputs may be any that keep to these rules, and one draw needn't show every extreme that they name: `comp_index`: positions of one list may repeat.
All inputs are finite; a program needn't handle non-finite values.
Results may differ from the reference program's by a relative error of at most 0.011.
Values may be sent and summed in bfloat16 or wider, within the bound.
A program may use at most 320 MiB of HBM per device.

```python
import jax
import jax.numpy as jnp
from jax import lax

D = 4096
FF = 7168
SPAN = 64
TOPK = 32
TOKENS = 1024
REPS = 4
N_REP = 4
N_TP = 8


def with_ends(drawn, key, least, largest):
    shape = drawn.shape
    spot = [jax.random.randint(jax.random.fold_in(key, axis), (), 0, shape[axis]) for axis in range(len(shape))]
    drawn = drawn.at[tuple(spot)].set(least)
    longest = shape.index(max(shape))
    spot[longest] = (spot[longest] + 1) % shape[longest]
    return drawn.at[tuple(spot)].set(largest)


def level_of(stream_key, shape, pieces, low, high):
    def one(dim, blocks):
        draws = jax.random.uniform(jax.random.fold_in(jax.random.fold_in(stream_key, 6), dim), (blocks,), jnp.float32, low / len(pieces), high / len(pieces))
        return jnp.repeat(jnp.exp(draws), shape[dim] // blocks).reshape((-1,) + (1,) * (len(shape) - dim - 1))

    level = one(*pieces[0])
    for cut in pieces[1:]:
        level = level * one(*cut)
    return level


def noise(key, extent, scale, bound, cuts=(), kind=jnp.bfloat16):
    drawn = scale * jax.random.normal(key, extent, jnp.float32)
    if cuts:
        drawn = drawn * level_of(key, extent, cuts, -0.22, 0.18)
    return jnp.clip(drawn, -bound, bound).astype(kind)


def setup_inputs(seed: int = 0) -> dict:
    keys = jax.random.split(jax.random.key(seed), 8)
    return {
        "residual": noise(keys[0], (REPS, TOKENS, D), 1.0, 6.0, ((0, 4), (1, 8))),
        "gate_pre": noise(keys[1], (REPS, TOKENS, FF), 1.0, 6.0, ((0, 4), (2, 8))),
        "up_pre": noise(keys[2], (REPS, TOKENS, FF), 1.0, 6.0, ((0, 4), (2, 8))),
        "down_weight": noise(keys[3], (FF, D), FF ** -0.5, 0.0625, ((0, 8),)),
        "d_out": noise(keys[4], (REPS, TOKENS, D), 0.25, 1.5, ((0, 4), (1, 8))),
        "comp_index": with_ends(jax.random.randint(keys[5], (REPS, FF // SPAN, (D // SPAN) * TOPK), 0, SPAN * SPAN), jax.random.fold_in(keys[5], 1), 0, (SPAN * SPAN) - 1).astype(jnp.int32),
        "comp_value": noise(keys[6], (REPS, FF // SPAN, (D // SPAN) * TOPK), 8.0, 48.0, ((0, 4), (1, 8))),
    }


def cosine_table(length):
    freq = jnp.arange(length, dtype=jnp.float32)[:, None]
    place = jnp.arange(length, dtype=jnp.float32)[None, :]
    scales = jnp.where(freq == 0, jnp.sqrt(1.0 / length), jnp.sqrt(2.0 / length))
    return scales * jnp.cos(jnp.pi * (2.0 * place + 1.0) * freq / (2.0 * length))

def reference(residual, gate_pre, up_pre, down_weight, d_out, comp_index, comp_value):
    units = FF // N_TP

    def per_replica(operands):
        residual_r, gate_r, up_r, grads_r = operands
        gate_f = gate_r.astype(jnp.float32)
        up_f = up_r.astype(jnp.float32)
        sigmoid_g = jax.nn.sigmoid(gate_f)
        activated = gate_f * sigmoid_g
        hidden = (activated * up_f).astype(jnp.bfloat16)
        summed = jnp.zeros((TOKENS, D), jnp.float32)
        for shard in range(N_TP):
            partial_out = jnp.dot(hidden[:, shard * units:(shard + 1) * units], down_weight[shard * units:(shard + 1) * units], preferred_element_type=jnp.float32)
            summed = summed + lax.optimization_barrier(partial_out.astype(jnp.bfloat16)).astype(jnp.float32)
        output = (residual_r.astype(jnp.float32) + summed).astype(jnp.bfloat16)
        hidden_grad = jnp.dot(grads_r, down_weight.T, preferred_element_type=jnp.float32)
        gate_preact_gradient = (hidden_grad * up_f * sigmoid_g * (1.0 + gate_f * (1.0 - sigmoid_g))).astype(jnp.bfloat16)
        up_grad = (hidden_grad * activated).astype(jnp.bfloat16)
        weight_grad = jnp.dot(hidden.T, grads_r, preferred_element_type=jnp.float32).astype(jnp.bfloat16)
        return (output, gate_preact_gradient, up_grad, weight_grad)
    output, gate_preact_gradient, up_grad, weight_grad = lax.map(per_replica, (residual, gate_pre, up_pre, d_out))
    cosine_basis = cosine_table(SPAN)
    columns = D // SPAN
    owners = jnp.broadcast_to((jnp.arange(columns * TOPK) // TOPK).astype(jnp.int32)[None, :], (N_REP, columns * TOPK))

    def span_row(operands):
        indices, amounts = operands
        flat = jnp.zeros((columns, SPAN * SPAN), jnp.float32).at[owners, indices.astype(jnp.int32)].add(amounts.astype(jnp.float32))
        spectral_coefficients = flat.reshape(columns, SPAN, SPAN)
        halfway_finished = jnp.einsum('kxt,ta->kxa', spectral_coefficients, cosine_basis, precision=lax.Precision.HIGHEST)
        output_block_list = jnp.einsum('nk,hnm->khm', cosine_basis, halfway_finished, precision=lax.Precision.HIGHEST)
        return output_block_list.reshape(SPAN, D)
    decoded = lax.map(span_row, (jnp.transpose(comp_index, (1, 0, 2)), jnp.transpose(comp_value, (1, 0, 2))))
    update = (decoded.reshape(FF, D) / N_REP).astype(jnp.bfloat16)
    updated_down_weight = (down_weight.astype(jnp.float32) - 0.02 * update.astype(jnp.float32)).astype(jnp.bfloat16)
    return (output, gate_preact_gradient, up_grad, weight_grad, update, updated_down_weight)
```

```python
import functools

import jax
import jax.numpy as jnp
import numpy as np
from jax import lax
from jax.experimental import pallas as pl
from jax.experimental.pallas import tpu as pltpu
from jax.sharding import PartitionSpec as P

SPAN = 64
TOPK = 32


learn_rate = 0.02


LANES = 128
UNROLL = 4
MESH = pl.DeviceIdType.MESH
VMEM_BYTES = 66_000_000
CHUNKS = 4


def cosine_table(length):
    freq = np.arange(length, dtype=np.float64)[:, None]
    place = np.arange(length, dtype=np.float64)[None, :]
    scales = np.where(freq == 0, np.sqrt(1.0 / length), np.sqrt(2.0 / length))
    return scales * np.cos(np.pi * (2.0 * place + 1.0) * freq / (2.0 * length))


def decode_kernel(count, *refs):
    index_refs, value_refs = refs[:count], refs[count:2 * count]
    weight_ref, right_ref, left_ref, update_ref, weight_out_ref, mixed_ref = refs[2 * count:]
    groups = index_refs[0].shape[1] // LANES
    per_group = LANES // TOPK
    width = per_group * SPAN
    depth = count * LANES
    lane = lax.broadcasted_iota(jnp.int32, (1, depth), 1)
    shift = ((lane // TOPK) % per_group) * SPAN
    row_place = lax.broadcasted_iota(jnp.int32, (SPAN, depth), 0).astype(jnp.float32).astype(jnp.bfloat16)
    col_place = lax.broadcasted_iota(jnp.int32, (width, depth), 0).astype(jnp.float32).astype(jnp.bfloat16)

    def gather(group, carry):
        at = pl.ds(pl.multiple_of(group * LANES, LANES), LANES)
        words = jnp.concatenate([ref[:, at] for ref in index_refs], axis=1)
        values = jnp.concatenate([ref[:, at] for ref in value_refs], axis=1).astype(jnp.bfloat16)
        rows = (words >> (SPAN.bit_length() - 1)).astype(jnp.float32).astype(jnp.bfloat16)
        cols = ((words & (SPAN - 1)) + shift).astype(jnp.float32).astype(jnp.bfloat16)
        row_hot = jnp.where(rows == row_place, values, jnp.bfloat16(0))
        col_hot = jnp.where(cols == col_place, jnp.bfloat16(1), jnp.bfloat16(0))
        spectral = lax.dot_general(
            row_hot, col_hot, (((1,), (1,)), ((), ())), preferred_element_type=jnp.float32
        )
        mixed_ref[pl.ds(pl.multiple_of(group * SPAN, SPAN), SPAN), :] = spectral.astype(jnp.bfloat16)
        return carry

    lax.fori_loop(0, groups, gather, 0, unroll=UNROLL)
    halfway = jnp.dot(
        mixed_ref[...], right_ref[...], preferred_element_type=jnp.float32
    ).astype(jnp.bfloat16)
    for group in range(groups):
        block = jnp.dot(
            left_ref[...], halfway[group * SPAN:(group + 1) * SPAN], preferred_element_type=jnp.float32
        )
        change = (block * (1.0 / count)).astype(jnp.bfloat16)
        at = slice(group * width, (group + 1) * width)
        update_ref[:, at] = change
        weight_out_ref[:, at] = (
            weight_ref[:, at].astype(jnp.float32) - learn_rate * change.astype(jnp.float32)
        ).astype(jnp.bfloat16)


def decode_tables():
    basis = cosine_table(SPAN)
    right = jnp.asarray(np.kron(np.eye(LANES // TOPK), basis), jnp.bfloat16)
    left = jnp.asarray(basis.T, jnp.bfloat16)
    return right, left


def decode(indices, values, down_weight):
    count = len(indices)
    span_rows, _, listed = indices[0].shape
    units, model = down_weight.shape
    per_group = LANES // TOPK
    width = per_group * SPAN
    right, left = decode_tables()
    strip = pl.BlockSpec((SPAN, model), lambda a: (a, 0))
    whole = lambda shape: pl.BlockSpec(shape, lambda a: (0, 0))
    return pl.pallas_call(
        functools.partial(decode_kernel, count),
        grid=(span_rows,),
        out_shape=[jax.ShapeDtypeStruct((units, model), jnp.bfloat16)] * 2,
        in_specs=[pl.BlockSpec((None, 1, listed), lambda a: (a, 0, 0))] * (2 * count)
        + [strip, whole((width, width)), whole((SPAN, SPAN))],
        out_specs=[strip, strip],
        scratch_shapes=[pltpu.VMEM((listed // LANES * SPAN, width), jnp.bfloat16)],
        compiler_params=pltpu.CompilerParams(
            dimension_semantics=("arbitrary",), vmem_limit_bytes=24 * 2**20
        ),
        cost_estimate=pl.CostEstimate(
            flops=20 * 10**9, bytes_accessed=units * model * 6, transcendentals=0
        ),
        name="decode",
    )(*indices, *values, down_weight, right, left)


def plain_shards(residual_r, gate_r, up_r, down_weight, grads_r, index_r, value_r):
    replicas = lax.axis_size("rep")

    def from_replicas(mine):
        return [mine] + [
            lax.ppermute(mine, "rep", [(i, (i + step) % replicas) for i in range(replicas)])
            for step in range(1, replicas)
        ]

    indices = from_replicas(index_r[:, None])
    values = from_replicas(value_r.astype(jnp.float32)[:, None])
    gate_f = gate_r.astype(jnp.float32)
    up_f = up_r.astype(jnp.float32)
    sigmoid_g = jax.nn.sigmoid(gate_f)
    activated = gate_f * sigmoid_g
    hidden = (activated * up_f).astype(jnp.bfloat16)
    summed = lax.psum_scatter(
        jnp.dot(hidden, down_weight, preferred_element_type=jnp.float32).astype(jnp.bfloat16),
        "tp",
        scatter_dimension=0,
        tiled=True,
    ).astype(jnp.float32)
    incoming = lax.all_gather(grads_r, "tp", axis=0, tiled=True)
    hidden_grad = lax.dot_general(
        incoming, down_weight, (((1,), (1,)), ((), ())), preferred_element_type=jnp.float32
    )
    weight_sum = lax.dot_general(
        hidden, incoming, (((0,), (0,)), ((), ())), preferred_element_type=jnp.float32
    )
    output = (residual_r.astype(jnp.float32) + summed).astype(jnp.bfloat16)
    gate_preact_gradient = (
        hidden_grad * up_f * sigmoid_g * (1.0 + gate_f * (1.0 - sigmoid_g))
    ).astype(jnp.bfloat16)
    up_grad = (hidden_grad * activated).astype(jnp.bfloat16)
    update, updated_down_weight = decode(indices, values, down_weight)
    return output, gate_preact_gradient, up_grad, weight_sum.astype(jnp.bfloat16), update, updated_down_weight


def rows_at(start, size):
    return pl.ds(pl.multiple_of(start, size), size)


def joint_kernel(
    n, replicas,
    residual, gate, up, weight, grads, index, value, right_ref, left_ref,
    output, gate_grad, up_grad, weight_grad, update, updated,
    dall, slot_up, slot_dn, part, peer, w_v, hidden, hidden_t, gate_v, up_v, res_v,
    index_v, value_v, row_v, col_v, amount_v, mixed, upd_st, new_st, gg_st, ug_st, wg_st, fin,
    load_sem, comp_send, comp_recv, step_send, step_recv, chip_send, chip_recv,
    part_send, part_recv, upd_sem, new_sem, gg_sem, ug_sem, wg_sem, out_sem,
):
    chips = n // 2
    rep = lax.axis_index("rep")
    me = lax.axis_index("tp")
    z, core = me // 2, me % 2
    partner = me + 1 - 2 * core
    tokens, units = gate_v.shape
    model = w_v.shape[1]
    block = tokens // n
    piece = block // CHUNKS
    span_rows, listed = index_v.shape[1], index_v.shape[2]
    groups = listed // LANES
    per_group = LANES // TOPK
    width = per_group * SPAN
    f32, bf16 = jnp.float32, jnp.bfloat16

    def cond(pred):
        return pl.when(pred)

    loads = [
        pltpu.make_async_copy(gate, gate_v, load_sem.at[0]),
        pltpu.make_async_copy(up, up_v, load_sem.at[1]),
        pltpu.make_async_copy(weight, w_v, load_sem.at[2]),
        pltpu.make_async_copy(grads, dall.at[rows_at(me * block, block)], load_sem.at[3]),
        pltpu.make_async_copy(index, index_v.at[rep], load_sem.at[4]),
        pltpu.make_async_copy(value, value_v.at[rep], load_sem.at[5]),
        pltpu.make_async_copy(residual, res_v, load_sem.at[6]),
    ]
    for load in loads:
        load.start()

    barrier = pltpu.get_barrier_semaphore()
    has_up, has_dn = z < chips - 1, z > 0

    @cond(has_up)
    def _():
        pl.semaphore_signal(barrier, inc=1, device_id={"tp": me + 2}, device_id_type=MESH)

    @cond(has_dn)
    def _():
        pl.semaphore_signal(barrier, inc=1, device_id={"tp": me - 2}, device_id_type=MESH)

    pl.semaphore_signal(barrier, inc=1, device_id={"tp": partner}, device_id_type=MESH)
    for step in range(1, replicas):
        pl.semaphore_signal(
            barrier, inc=1, device_id={"rep": (rep + step) % replicas}, device_id_type=MESH
        )
    pl.semaphore_wait(barrier, replicas + has_up.astype(jnp.int32) + has_dn.astype(jnp.int32))

    def send(way, s, src, dst):
        return pltpu.make_async_remote_copy(
            src_ref=src, dst_ref=dst, send_sem=step_send.at[way, s], recv_sem=step_recv.at[way, s],
            device_id={"tp": me + (2 if way == 0 else -2)}, device_id_type=MESH,
        )

    def grad_piece(chip, q):
        return dall.at[rows_at((2 * chip + core) * block + q * piece, piece)]

    def to_partner(chip, q):
        return pltpu.make_async_remote_copy(
            src_ref=grad_piece(chip, q), dst_ref=grad_piece(chip, q),
            send_sem=chip_send.at[chip * CHUNKS + q], recv_sem=chip_recv.at[chip * CHUNKS + q],
            device_id={"tp": partner}, device_id_type=MESH,
        )

    def hand_over(target):
        return pltpu.make_async_remote_copy(
            src_ref=part.at[rows_at((2 * target + 1 - core) * block, block)],
            dst_ref=peer.at[rows_at(target * block, block)],
            send_sem=part_send.at[target], recv_sem=part_recv.at[target],
            device_id={"tp": partner}, device_id_type=MESH,
        )

    def comp_copies(step):
        to = {"rep": (rep + step) % replicas}
        return [
            pltpu.make_async_remote_copy(
                src_ref=src, dst_ref=dst.at[rep], send_sem=comp_send.at[kind, step - 1],
                recv_sem=comp_recv.at[kind, step - 1], device_id=to, device_id_type=MESH,
            )
            for kind, (src, dst) in enumerate(((index, index_v), (value, value_v)))
        ]

    slots = (slot_up, slot_dn)
    rank = (z, chips - 1 - z)
    onward = (has_up, has_dn)
    behind = (has_dn, has_up)

    for q in range(CHUNKS):
        for way in range(2):
            @cond(onward[way])
            def _():
                send(way, q, grads.at[pl.ds(q * piece, piece)], grad_piece(z, q)).start()

    for step in range(1, replicas):
        for copy in comp_copies(step):
            copy.start()

    loads[3].wait()
    for q in range(CHUNKS):
        to_partner(z, q).start()

    def own_sum(target, q):
        mine = part[rows_at((2 * target + core) * block + q * piece, piece), :].astype(f32)
        other = peer[rows_at(target * block + q * piece, piece), :].astype(f32)
        return mine + other

    def slot_rows(p, q):
        return rows_at((p - 1) * block + q * piece, piece)

    def service(s):
        p, q = s // CHUNKS, s % CHUNKS
        for way in range(2):
            at, slot = rank[way], slots[way]
            gathered = p < at
            source = z - 1 - p if way == 0 else z + 1 + p
            target = chips + z - 1 - p if way == 0 else z - chips + 1 + p
            summing = jnp.logical_and(jnp.logical_and(p >= at, onward[way]), p < chips - 1)
            first = at == 0

            @cond(behind[way])
            def _():
                send(way, s, grad_piece(z, q), grad_piece(z, q)).wait_recv()

            @cond(gathered)
            def _():
                to_partner(source, q).start()

                @cond(onward[way])
                def _():
                    send(way, s + CHUNKS, grad_piece(source, q), grad_piece(source, q)).start()

            @cond(jnp.logical_and(summing, first))
            def _():
                slot[slot_rows(p + 1, q), :] = own_sum(target, q).astype(bf16)
                send(way, s + CHUNKS, slot.at[slot_rows(p + 1, q)], slot.at[slot_rows(p + 1, q)]).start()

            @cond(jnp.logical_and(summing, jnp.logical_not(first)))
            def _():
                here = slot_rows(p, q)
                slot[here, :] = (own_sum(target, q) + slot[here, :].astype(f32)).astype(bf16)
                send(way, s + CHUNKS, slot.at[here], slot.at[slot_rows(p + 1, q)]).start()

    def put_output(q):
        return pltpu.make_async_copy(fin_b.at[pl.ds(q * piece, piece)], output.at[pl.ds(q * piece, piece)], out_sem.at[q])

    fin_b = res_v

    def finish(q):
        here = pl.ds(q * piece, piece)
        fin[...] = res_v[here, :].astype(f32) + own_sum(z, q)
        for way in range(2):
            @cond(behind[way])
            def _():
                fin[...] = fin[...] + slots[way][pl.ds((chips - 2) * block + q * piece, piece), :].astype(f32)
        res_v[here, :] = fin[...].astype(bf16)
        put_output(q).start()

    loads[0].wait()
    loads[1].wait()

    def make_hidden(i, carry):
        here = rows_at(i * LANES, LANES)
        g = gate_v[here, :].astype(f32)
        u = up_v[here, :].astype(f32)
        h = (g * jax.nn.sigmoid(g) * u).astype(bf16)
        hidden[here, :] = h
        hidden_t[:, here] = h.astype(f32).T.astype(bf16)
        return carry

    lax.fori_loop(0, tokens // LANES, make_hidden, 0)

    loads[2].wait()
    tile = 512

    def make_part(i, carry):
        here = rows_at(i * tile, tile)
        part[:, here] = jnp.dot(hidden[...], w_v[:, here], preferred_element_type=f32).astype(bf16)
        return carry

    lax.fori_loop(0, model // tile, make_part, 0)
    order = []
    for k in range(chips):
        order.append(chips - 1 - k // 2 if k % 2 == 0 else k // 2)
    for target in order:
        hand_over(target).start()

    for step in range(1, replicas):
        for copy in comp_copies(step):
            copy.wait_recv()
    loads[4].wait()
    loads[5].wait()
    pairs = replicas // 2
    half = LANES // 2
    spot = lax.broadcasted_iota(jnp.int32, (span_rows, listed), 1)
    lower = spot % LANES < half
    shift = ((spot // TOPK) % 2) * SPAN

    def spread_out(dest, arrays):
        for j in range(pairs):
            even, odd = arrays[2 * j], arrays[2 * j + 1]
            first = jnp.where(lower, even, pltpu.roll(odd, half, 1))
            second = jnp.where(lower, pltpu.roll(even, listed - half, 1), odd)
            for a in range(span_rows):
                dest[a, j:j + 1, :] = first[a:a + 1]
                dest[a, pairs + j:pairs + j + 1, :] = second[a:a + 1]

    spread_out(row_v, [(index_v[r] >> (SPAN.bit_length() - 1)).astype(f32) for r in range(replicas)])
    spread_out(col_v, [((index_v[r] & (SPAN - 1)) + shift).astype(f32) for r in range(replicas)])
    spread_out(amount_v, [value_v[r].astype(f32) for r in range(replicas)])
    deep = pairs * LANES
    row_place = lax.broadcasted_iota(jnp.int32, (SPAN, deep), 0).astype(f32).astype(bf16)
    col_place = lax.broadcasted_iota(jnp.int32, (2 * SPAN, deep), 0).astype(f32).astype(bf16)

    def put_update(a, k):
        rows = rows_at(a * SPAN, SPAN)
        return (
            pltpu.make_async_copy(upd_st.at[k], update.at[rows], upd_sem.at[k]),
            pltpu.make_async_copy(new_st.at[k], updated.at[rows], new_sem.at[k]),
        )

    def decode_row(a):
        k = a % 2

        @cond(a >= 2)
        def _():
            for copy in put_update(a, k):
                copy.wait()

        def gather(group, carry):
            at = rows_at(group * LANES, LANES)
            row_set, col_set, amount_set = row_v[a, :, at], col_v[a, :, at], amount_v[a, :, at]
            for side in range(2):
                line = lambda x: jnp.concatenate(
                    [x[side * pairs + j:side * pairs + j + 1] for j in range(pairs)], axis=1
                ).astype(bf16)
                row_hot = jnp.where(line(row_set) == row_place, line(amount_set), bf16(0))
                col_hot = jnp.where(line(col_set) == col_place, bf16(1), bf16(0))
                spectral = lax.dot_general(
                    row_hot, col_hot, (((1,), (1,)), ((), ())), preferred_element_type=f32
                )
                mixed[rows_at(group * SPAN, SPAN), side * 2 * SPAN:(side + 1) * 2 * SPAN] = spectral.astype(bf16)
            return carry

        lax.fori_loop(0, groups, gather, 0, unroll=UNROLL)
        halfway = jnp.dot(mixed[...], right_ref[...], preferred_element_type=f32).astype(bf16)
        for group in range(groups):
            spread = jnp.dot(
                left_ref[...], halfway[group * SPAN:(group + 1) * SPAN], preferred_element_type=f32
            )
            change = (spread * (1.0 / replicas)).astype(bf16)
            at = slice(group * width, (group + 1) * width)
            upd_st[k, :, at] = change
            new_st[k, :, at] = (
                w_v[rows_at(a * SPAN, SPAN), at].astype(f32) - learn_rate * change.astype(f32)
            ).astype(bf16)
        for copy in put_update(a, k):
            copy.start()

    early = CHUNKS - 1
    decode_head = 2

    def decode_step(a, carry):
        decode_row(a)

        @cond(a == decode_head - 1)
        def _():
            for target in order:
                hand_over(target).wait_recv()
            for s in range(early):
                service(s)

        @cond(jnp.logical_and(a >= decode_head, a % 2 == 1))
        def _():
            service(early + (a - decode_head) // 2)

        return carry

    lax.fori_loop(0, span_rows, decode_step, 0)
    served = early + (span_rows - decode_head) // 2
    for k in range(2):
        for copy in put_update(span_rows - 2 + k, k):
            copy.wait()

    def serve_to(start, stop):
        if stop > start:
            lax.fori_loop(start, stop, lambda s, carry: (service(s), carry)[1], 0)

    low = z < chips // 2

    def put_grads(start, k):
        rows = rows_at(start, 2 * block)
        return (
            pltpu.make_async_copy(gg_st.at[k], gate_grad.at[rows], gg_sem.at[k]),
            pltpu.make_async_copy(ug_st.at[k], up_grad.at[rows], ug_sem.at[k]),
        )

    def wait_chip(chip):
        for q in range(CHUNKS):
            to_partner(chip, q).wait_recv()

    def chip_at(k):
        return jnp.where(low, k, chips - 1 - k)

    def grads_of(k, carry):
        chip = chip_at(k)
        start = chip * 2 * block
        wait_chip(chip)
        j = k % 2

        @cond(k >= 2)
        def _():
            for copy in put_grads(start, j):
                copy.wait()

        rows = rows_at(start, 2 * block)
        back = lax.dot_general(
            dall[rows, :], w_v[...], (((1,), (1,)), ((), ())), preferred_element_type=f32
        )
        g = gate_v[rows, :].astype(f32)
        u = up_v[rows, :].astype(f32)
        sig = jax.nn.sigmoid(g)
        gg_st[j] = (back * u * sig * (1.0 + g * (1.0 - sig))).astype(bf16)
        ug_st[j] = (back * (g * sig)).astype(bf16)
        for copy in put_grads(start, j):
            copy.start()
        return carry

    serve_to(served, 2 * CHUNKS + 1)
    lax.fori_loop(0, chips // 2, grads_of, 0)
    serve_to(2 * CHUNKS + 1, (chips - 1) * CHUNKS)
    lax.fori_loop(chips // 2, chips, grads_of, 0)

    wide = 256
    last = (chips - 1) * CHUNKS
    service(last)
    loads[6].wait()
    finish(0)

    def put_weight(i, k):
        return pltpu.make_async_copy(wg_st.at[k], weight_grad.at[:, rows_at(i * wide, wide)], wg_sem.at[k])

    def make_weight(i, carry):
        k = i % 2

        @cond(i >= 2)
        def _():
            put_weight(i, k).wait()

        wg_st[k] = jnp.dot(
            hidden_t[...], dall[:, rows_at(i * wide, wide)], preferred_element_type=f32
        ).astype(bf16)
        put_weight(i, k).start()
        return carry

    turns = model // wide
    marks = [turns * k // (CHUNKS - 1) for k in range(CHUNKS)]
    for q in range(1, CHUNKS):
        lax.fori_loop(marks[q - 1], marks[q], make_weight, 0)
        service(last + q)
        finish(q)

    for k in range(2):
        put_weight(turns - 2 + k, k).wait()
        for copy in put_grads(0, k):
            copy.wait()
    for q in range(CHUNKS):
        put_output(q).wait()
    for target in range(chips):
        hand_over(target).wait_send()
    for chip in range(chips):
        for q in range(CHUNKS):
            to_partner(chip, q).wait_send()
    for step in range(1, replicas):
        for copy in comp_copies(step):
            copy.wait_send()
    for way in range(2):
        @cond(onward[way])
        def _():
            for s in range(chips * CHUNKS):
                send(way, s, grad_piece(z, 0), grad_piece(z, 0)).wait_send()


def joint_scratch(n, replicas, tokens, units, model, span_rows, listed):
    chips, block = n // 2, tokens // n
    bf16, f32 = jnp.bfloat16, jnp.float32
    dma = pltpu.SemaphoreType.DMA
    arrays = [
        ((tokens, model), bf16),
        (((chips - 1) * block, model), bf16),
        (((chips - 1) * block, model), bf16),
        ((tokens, model), bf16),
        ((chips * block, model), bf16),
        ((units, model), bf16),
        ((tokens, units), bf16),
        ((units, tokens), bf16),
        ((tokens, units), bf16),
        ((tokens, units), bf16),
        ((block, model), bf16),
        ((replicas, span_rows, listed), jnp.int32),
        ((replicas, span_rows, listed), bf16),
        ((span_rows, replicas, listed), f32),
        ((span_rows, replicas, listed), f32),
        ((span_rows, replicas, listed), f32),
        ((listed // LANES * SPAN, LANES // TOPK * SPAN), bf16),
        ((2, SPAN, model), bf16),
        ((2, SPAN, model), bf16),
        ((2, 2 * block, units), bf16),
        ((2, 2 * block, units), bf16),
        ((2, units, 256), bf16),
        ((block // CHUNKS, model), f32),
    ]
    total = sum(int(np.prod(shape)) * jnp.dtype(kind).itemsize for shape, kind in arrays)
    steps = chips * CHUNKS
    sems = [
        dma((7,)), dma((2, replicas - 1)), dma((2, replicas - 1)), dma((2, steps)), dma((2, steps)),
        dma((steps,)), dma((steps,)), dma((chips,)), dma((chips,)),
        dma((2,)), dma((2,)), dma((2,)), dma((2,)), dma((2,)), dma((CHUNKS,)),
    ]
    return total, [pltpu.VMEM(shape, kind) for shape, kind in arrays] + sems


def joint(residual_r, gate_r, up_r, down_weight, grads_r, index_r, value_r, scratch):
    n, replicas = lax.axis_size("tp"), lax.axis_size("rep")
    (tokens, units), model = gate_r.shape, down_weight.shape[1]
    right, left = decode_tables()
    any_spec = pl.BlockSpec(memory_space=pl.ANY)
    vmem_spec = pl.BlockSpec(memory_space=pltpu.VMEM)
    shape = lambda *dims: jax.ShapeDtypeStruct(dims, jnp.bfloat16)
    return pl.pallas_call(
        functools.partial(joint_kernel, n, replicas),
        out_shape=[
            shape(*residual_r.shape), shape(tokens, units), shape(tokens, units),
            shape(units, model), shape(units, model), shape(units, model),
        ],
        in_specs=[any_spec] * 7 + [vmem_spec] * 2,
        out_specs=[any_spec] * 6,
        scratch_shapes=scratch,
        compiler_params=pltpu.CompilerParams(
            collective_id=0, has_side_effects=True, vmem_limit_bytes=VMEM_BYTES
        ),
        cost_estimate=pl.CostEstimate(
            flops=6 * tokens * units * model, bytes_accessed=units * model * 8, transcendentals=0
        ),
        name="joint",
    )(residual_r, gate_r, up_r, down_weight, grads_r, index_r, value_r, right, left)


def shards(residual, gate_pre, up_pre, down_weight, d_out, comp_index, comp_value):
    operands = (residual[0], gate_pre[0], up_pre[0], down_weight, d_out[0], comp_index[0], comp_value[0])
    n, replicas = lax.axis_size("tp"), lax.axis_size("rep")
    tokens, units = gate_pre.shape[1:]
    span_rows, listed = comp_index.shape[1:]
    model = down_weight.shape[1]
    fits = False
    if n % 4 == 0 and units % LANES == 0 and span_rows % 2 == 0 and replicas % 2 == 0:
        total, scratch = joint_scratch(n, replicas, tokens, units, model, span_rows, listed)
        fits = total < 56 * 2**20 and n // 2 == CHUNKS
    if fits:
        outs = joint(*operands, scratch)
    else:
        outs = plain_shards(*operands)
    output, gate_preact_gradient, up_grad, weight_sum, update, updated = outs
    return (
        output[None],
        gate_preact_gradient[None],
        up_grad[None],
        weight_sum[None],
        update,
        updated,
    )


def solution(mesh):
    return jax.shard_map(
        shards,
        mesh=mesh,
        in_specs=(
            P("rep", "tp", None),
            P("rep", None, "tp"),
            P("rep", None, "tp"),
            P("tp", None),
            P("rep", "tp", None),
            P("rep", "tp", None),
            P("rep", "tp", None),
        ),
        out_specs=(
            P("rep", "tp", None),
            P("rep", None, "tp"),
            P("rep", None, "tp"),
            P("rep", "tp", None),
            P("tp", None),
            P("tp", None),
        ),
        check_vma=False,
    )
```

```python
import functools

import jax
import jax.numpy as jnp
import numpy as np
from jax import lax
from jax.experimental import pallas as pl
from jax.experimental.pallas import tpu as pltpu
from jax.sharding import PartitionSpec as P

SPAN = 64
TOPK = 32


learn_rate = 0.02


LANES = 128
UNROLL = 4
MESH = pl.DeviceIdType.MESH
VMEM_BYTES = 37 * 2**20
PUT_BYTES = 2**20
CHUNKS = 4
FIRST = 2


def cosine_table(length):
    freq = np.arange(length, dtype=np.float64)[:, None]
    place = np.arange(length, dtype=np.float64)[None, :]
    scales = np.where(freq == 0, np.sqrt(1.0 / length), np.sqrt(2.0 / length))
    return scales * np.cos(np.pi * (2.0 * place + 1.0) * freq / (2.0 * length))


def decode_kernel(count, *refs):
    index_refs, value_refs = refs[:count], refs[count:2 * count]
    weight_ref, right_ref, left_ref, update_ref, weight_out_ref, mixed_ref = refs[2 * count:]
    groups = index_refs[0].shape[1] // LANES
    per_group = LANES // TOPK
    width = per_group * SPAN
    depth = count * LANES
    lane = lax.broadcasted_iota(jnp.int32, (1, depth), 1)
    shift = ((lane // TOPK) % per_group) * SPAN
    row_place = lax.broadcasted_iota(jnp.int32, (SPAN, depth), 0).astype(jnp.float32).astype(jnp.bfloat16)
    col_place = lax.broadcasted_iota(jnp.int32, (width, depth), 0).astype(jnp.float32).astype(jnp.bfloat16)

    def gather(group, carry):
        at = pl.ds(pl.multiple_of(group * LANES, LANES), LANES)
        words = jnp.concatenate([ref[:, at] for ref in index_refs], axis=1)
        values = jnp.concatenate([ref[:, at] for ref in value_refs], axis=1).astype(jnp.bfloat16)
        rows = (words >> (SPAN.bit_length() - 1)).astype(jnp.float32).astype(jnp.bfloat16)
        cols = ((words & (SPAN - 1)) + shift).astype(jnp.float32).astype(jnp.bfloat16)
        row_hot = jnp.where(rows == row_place, values, jnp.bfloat16(0))
        col_hot = jnp.where(cols == col_place, jnp.bfloat16(1), jnp.bfloat16(0))
        spectral = lax.dot_general(
            row_hot, col_hot, (((1,), (1,)), ((), ())), preferred_element_type=jnp.float32
        )
        mixed_ref[pl.ds(pl.multiple_of(group * SPAN, SPAN), SPAN), :] = spectral.astype(jnp.bfloat16)
        return carry

    lax.fori_loop(0, groups, gather, 0, unroll=UNROLL)
    halfway = jnp.dot(
        mixed_ref[...], right_ref[...], preferred_element_type=jnp.float32
    ).astype(jnp.bfloat16)
    for group in range(groups):
        block = jnp.dot(
            left_ref[...], halfway[group * SPAN:(group + 1) * SPAN], preferred_element_type=jnp.float32
        )
        change = (block * (1.0 / count)).astype(jnp.bfloat16)
        at = slice(group * width, (group + 1) * width)
        update_ref[:, at] = change
        weight_out_ref[:, at] = (
            weight_ref[:, at].astype(jnp.float32) - learn_rate * change.astype(jnp.float32)
        ).astype(jnp.bfloat16)


def decode_tables():
    basis = cosine_table(SPAN)
    right = jnp.asarray(np.kron(np.eye(LANES // TOPK), basis), jnp.bfloat16)
    left = jnp.asarray(basis.T, jnp.bfloat16)
    return right, left


def decode(indices, values, down_weight):
    count = len(indices)
    span_rows, _, listed = indices[0].shape
    units, model = down_weight.shape
    per_group = LANES // TOPK
    width = per_group * SPAN
    right, left = decode_tables()
    strip = pl.BlockSpec((SPAN, model), lambda a: (a, 0))
    whole = lambda shape: pl.BlockSpec(shape, lambda a: (0, 0))
    return pl.pallas_call(
        functools.partial(decode_kernel, count),
        grid=(span_rows,),
        out_shape=[jax.ShapeDtypeStruct((units, model), jnp.bfloat16)] * 2,
        in_specs=[pl.BlockSpec((None, 1, listed), lambda a: (a, 0, 0))] * (2 * count)
        + [strip, whole((width, width)), whole((SPAN, SPAN))],
        out_specs=[strip, strip],
        scratch_shapes=[pltpu.VMEM((listed // LANES * SPAN, width), jnp.bfloat16)],
        compiler_params=pltpu.CompilerParams(
            dimension_semantics=("arbitrary",), vmem_limit_bytes=24 * 2**20
        ),
        cost_estimate=pl.CostEstimate(
            flops=20 * 10**9, bytes_accessed=units * model * 6, transcendentals=0
        ),
        name="decode",
    )(*indices, *values, down_weight, right, left)


def plain_shards(residual_r, gate_r, up_r, down_weight, grads_r, index_r, value_r):
    replicas = lax.axis_size("rep")

    def from_replicas(mine):
        return [mine] + [
            lax.ppermute(mine, "rep", [(i, (i + step) % replicas) for i in range(replicas)])
            for step in range(1, replicas)
        ]

    indices = from_replicas(index_r[:, None])
    values = from_replicas(value_r.astype(jnp.float32)[:, None])
    gate_f = gate_r.astype(jnp.float32)
    up_f = up_r.astype(jnp.float32)
    sigmoid_g = jax.nn.sigmoid(gate_f)
    activated = gate_f * sigmoid_g
    hidden = (activated * up_f).astype(jnp.bfloat16)
    summed = lax.psum_scatter(
        jnp.dot(hidden, down_weight, preferred_element_type=jnp.float32).astype(jnp.bfloat16),
        "tp",
        scatter_dimension=0,
        tiled=True,
    ).astype(jnp.float32)
    incoming = lax.all_gather(grads_r, "tp", axis=0, tiled=True)
    hidden_grad = lax.dot_general(
        incoming, down_weight, (((1,), (1,)), ((), ())), preferred_element_type=jnp.float32
    )
    weight_sum = lax.dot_general(
        hidden, incoming, (((0,), (0,)), ((), ())), preferred_element_type=jnp.float32
    )
    output = (residual_r.astype(jnp.float32) + summed).astype(jnp.bfloat16)
    gate_preact_gradient = (
        hidden_grad * up_f * sigmoid_g * (1.0 + gate_f * (1.0 - sigmoid_g))
    ).astype(jnp.bfloat16)
    up_grad = (hidden_grad * activated).astype(jnp.bfloat16)
    update, updated_down_weight = decode(indices, values, down_weight)
    return output, gate_preact_gradient, up_grad, weight_sum.astype(jnp.bfloat16), update, updated_down_weight


def rows_at(start, size):
    return pl.ds(pl.multiple_of(start, size), size)


def joint_kernel(
    n, replicas,
    residual, gate, up, weight, grads, index, value, right_ref, left_ref,
    output, gate_grad, up_grad, weight_grad, update, updated,
    dall, slot_up, slot_dn, part, w_v, hidden, hidden_t,
    index_v, value_v, word_v, amount_v, mixed, fin,
    load_sem, comp_send, comp_recv, step_send, step_recv, chip_send, chip_recv,
    part_send, part_recv,
):
    chips = n // 2
    rep = lax.axis_index("rep")
    me = lax.axis_index("tp")
    z, core = me // 2, me % 2
    partner = me + 1 - 2 * core
    tokens, units = gate_grad.shape
    model = w_v.shape[1]
    block = tokens // n
    piece = block // CHUNKS
    span_rows, listed = value_v.shape[1], value_v.shape[2]
    groups = listed // LANES
    per_group = LANES // TOPK
    width = per_group * SPAN
    f32, bf16 = jnp.float32, jnp.bfloat16

    loads = [
        pltpu.make_async_copy(gate, gate_grad, load_sem.at[0]),
        pltpu.make_async_copy(up, up_grad, load_sem.at[1]),
        pltpu.make_async_copy(weight, w_v, load_sem.at[2]),
        pltpu.make_async_copy(grads, dall.at[rows_at(me * block, block)], load_sem.at[3]),
        pltpu.make_async_copy(index, index_v.at[rep], load_sem.at[4]),
        pltpu.make_async_copy(value, value_v.at[rep], load_sem.at[5]),
        pltpu.make_async_copy(residual, output, load_sem.at[6]),
    ]
    for load in loads:
        load.start()

    barrier = pltpu.get_barrier_semaphore()
    has_up, has_dn = z < chips - 1, z > 0

    @pl.when(has_up)
    def _():
        pl.semaphore_signal(barrier, inc=1, device_id={"tp": me + 2}, device_id_type=MESH)

    @pl.when(has_dn)
    def _():
        pl.semaphore_signal(barrier, inc=1, device_id={"tp": me - 2}, device_id_type=MESH)

    pl.semaphore_signal(barrier, inc=1, device_id={"tp": partner}, device_id_type=MESH)
    for step in range(1, replicas):
        pl.semaphore_signal(
            barrier, inc=1, device_id={"rep": (rep + step) % replicas}, device_id_type=MESH
        )
    pl.semaphore_wait(barrier, replicas + has_up.astype(jnp.int32) + has_dn.astype(jnp.int32))

    def send(way, s, src, dst):
        return pltpu.make_async_remote_copy(
            src_ref=src, dst_ref=dst, send_sem=step_send.at[way, s], recv_sem=step_recv.at[way, s],
            device_id={"tp": me + (2 if way == 0 else -2)}, device_id_type=MESH,
        )

    def grad_piece(chip, q):
        return dall.at[rows_at((2 * chip + core) * block + q * piece, piece)]

    def to_partner(chip, q):
        return pltpu.make_async_remote_copy(
            src_ref=grad_piece(chip, q), dst_ref=grad_piece(chip, q),
            send_sem=chip_send.at[chip * CHUNKS + q], recv_sem=chip_recv.at[chip * CHUNKS + q],
            device_id={"tp": partner}, device_id_type=MESH,
        )

    lent = units - chips * block

    def hand_over(target):
        return pltpu.make_async_remote_copy(
            src_ref=update.at[pl.ds(lent + target * block, block)],
            dst_ref=weight_grad.at[pl.ds(target * block, block)],
            send_sem=part_send.at[target], recv_sem=part_recv.at[target],
            device_id={"tp": partner}, device_id_type=MESH,
        )

    def comp_copies(step):
        to = {"rep": (rep + step) % replicas}
        return [
            pltpu.make_async_remote_copy(
                src_ref=src, dst_ref=dst.at[rep], send_sem=comp_send.at[kind, step - 1],
                recv_sem=comp_recv.at[kind, step - 1], device_id=to, device_id_type=MESH,
            )
            for kind, (src, dst) in enumerate(((index, index_v), (value, value_v)))
        ]

    slots = (slot_up, slot_dn)
    rank = (z, chips - 1 - z)
    onward = (has_up, has_dn)
    behind = (has_dn, has_up)

    for q in range(CHUNKS):
        for way in range(2):
            @pl.when(onward[way])
            def _():
                send(way, q, grads.at[pl.ds(q * piece, piece)], grad_piece(z, q)).start()

    for step in range(1, replicas):
        for copy in comp_copies(step):
            copy.start()

    loads[3].wait()
    for q in range(CHUNKS):
        to_partner(z, q).start()

    def own_sum(target, q):
        return part[rows_at(target * block + q * piece, piece), :]

    def slot_rows(p, q):
        return rows_at((p - 1) * block + q * piece, piece)

    def service(s):
        p, q = s // CHUNKS, s % CHUNKS
        for way in range(2):
            at, slot = rank[way], slots[way]
            gathered = p < at
            source = z - 1 - p if way == 0 else z + 1 + p
            target = chips + z - 1 - p if way == 0 else z - chips + 1 + p
            summing = jnp.logical_and(jnp.logical_and(p >= at, onward[way]), p < chips - 1)
            first = at == 0

            @pl.when(behind[way])
            def _():
                send(way, s, grad_piece(z, q), grad_piece(z, q)).wait_recv()

            @pl.when(gathered)
            def _():
                to_partner(source, q).start()

                @pl.when(onward[way])
                def _():
                    send(way, s + CHUNKS, grad_piece(source, q), grad_piece(source, q)).start()

            @pl.when(jnp.logical_and(summing, first))
            def _():
                mine = part.at[rows_at(target * block + q * piece, piece)]
                send(way, s + CHUNKS, mine, slot.at[slot_rows(p + 1, q)]).start()

            @pl.when(jnp.logical_and(summing, jnp.logical_not(first)))
            def _():
                here = slot_rows(p, q)
                slot[here, :] = (own_sum(target, q).astype(f32) + slot[here, :].astype(f32)).astype(bf16)
                send(way, s + CHUNKS, slot.at[here], slot.at[slot_rows(p + 1, q)]).start()

    def finish(q):
        here = pl.ds(q * piece, piece)
        fin[...] = output[here, :].astype(f32) + own_sum(z, q).astype(f32)
        for way in range(2):
            @pl.when(behind[way])
            def _():
                fin[...] = fin[...] + slots[way][pl.ds((chips - 2) * block + q * piece, piece), :].astype(f32)
        output[here, :] = fin[...].astype(bf16)

    loads[0].wait()
    loads[1].wait()

    def make_hidden(i, carry):
        here = rows_at(i * block, block)
        g = gate_grad[here, :].astype(f32)
        u = up_grad[here, :].astype(f32)
        h = (g * jax.nn.sigmoid(g) * u).astype(bf16)
        hidden[here, :] = h
        hidden_t[:, here] = h.astype(f32).T.astype(bf16)
        return carry

    tile = 512

    def target_at(k):
        return jnp.where(k % 2 == 0, chips - 1 - k // 2, k // 2)

    def add_other(k):
        target = target_at(k)
        hand_over(target).wait_recv()

        def add_part(q, carry):
            here = rows_at(target * block + q * piece, piece)
            part[here, :] = (part[here, :].astype(f32) + weight_grad[here, :].astype(f32)).astype(bf16)
            return carry

        lax.fori_loop(0, CHUNKS, add_part, 0)

    def make_target(k, carry):
        target = target_at(k)
        lax.fori_loop(2 * target, 2 * target + 2, make_hidden, 0)
        rows = rows_at(2 * target * block, 2 * block)
        mine, other = rows_at(target * block, block), rows_at(lent + target * block, block)

        def make_part(i, carry):
            here = rows_at(i * tile, tile)
            got = jnp.dot(hidden[rows, :], w_v[:, here], preferred_element_type=f32).astype(bf16)

            @pl.when(core == 0)
            def _():
                part[mine, here] = got[:block]
                update[other, here] = got[block:]

            @pl.when(core == 1)
            def _():
                part[mine, here] = got[block:]
                update[other, here] = got[:block]
            return carry

        lax.fori_loop(0, model // tile, make_part, 0)
        hand_over(target).start()

        @pl.when(k > 0)
        def _():
            add_other(k - 1)

        @pl.when(k >= FIRST)
        def _():
            service(k - FIRST)

        return carry

    loads[2].wait()
    lax.fori_loop(0, chips, make_target, 0)

    for step in range(1, replicas):
        for copy in comp_copies(step):
            copy.wait_recv()
    loads[4].wait()
    loads[5].wait()

    pairs = replicas // 2
    half = LANES // 2
    spot = lax.broadcasted_iota(jnp.int32, (1, listed), 1)
    lower = spot % LANES < half
    for a in range(span_rows):
        for j in range(pairs):
            for dest, pick in (
                (word_v, lambda r: index_v[r, a]),
                (amount_v, lambda r: value_v[r].astype(f32)[a:a + 1]),
            ):
                even, odd = pick(2 * j), pick(2 * j + 1)
                dest[a, j:j + 1, :] = jnp.where(lower, even, pltpu.roll(odd, half, 1))
                dest[a, pairs + j:pairs + j + 1, :] = jnp.where(lower, pltpu.roll(even, listed - half, 1), odd)

    deep = pairs * LANES
    shift = ((lax.broadcasted_iota(jnp.int32, (replicas, LANES), 1) // TOPK) % 2) * SPAN
    row_place = lax.broadcasted_iota(jnp.int32, (SPAN, deep), 0).astype(f32).astype(bf16)
    col_place = lax.broadcasted_iota(jnp.int32, (2 * SPAN, deep), 0).astype(f32).astype(bf16)

    def decode_row(a):
        def gather(group, carry):
            at = rows_at(group * LANES, LANES)
            words = word_v[a, :, at]
            row_set = (words >> (SPAN.bit_length() - 1)).astype(f32)
            col_set = ((words & (SPAN - 1)) + shift).astype(f32)
            amount_set = amount_v[a, :, at]
            for side in range(2):
                line = lambda x: jnp.concatenate(
                    [x[side * pairs + j:side * pairs + j + 1] for j in range(pairs)], axis=1
                ).astype(bf16)
                row_hot = jnp.where(line(row_set) == row_place, line(amount_set), bf16(0))
                col_hot = jnp.where(line(col_set) == col_place, bf16(1), bf16(0))
                spectral = lax.dot_general(
                    row_hot, col_hot, (((1,), (1,)), ((), ())), preferred_element_type=f32
                )
                mixed[rows_at(group * SPAN, SPAN), side * 2 * SPAN:(side + 1) * 2 * SPAN] = spectral.astype(bf16)
            return carry

        lax.fori_loop(0, groups, gather, 0, unroll=UNROLL)
        halfway = jnp.dot(mixed[...], right_ref[...], preferred_element_type=f32).astype(bf16)
        rows = rows_at(a * SPAN, SPAN)
        for group in range(groups):
            spread = jnp.dot(
                left_ref[...], halfway[group * SPAN:(group + 1) * SPAN], preferred_element_type=f32
            )
            change = (spread * (1.0 / replicas)).astype(bf16)
            at = slice(group * width, (group + 1) * width)
            update[rows, at] = change
            updated[rows, at] = (w_v[rows, at].astype(f32) - learn_rate * change.astype(f32)).astype(bf16)

    def decode_step(a, carry):
        decode_row(a)

        @pl.when(a % 2 == 1)
        def _():
            service(chips - FIRST + a // 2)

        return carry

    add_other(chips - 1)
    for target in range(chips):
        hand_over(target).wait_send()
    lax.fori_loop(0, span_rows, decode_step, 0)
    served = chips - FIRST + span_rows // 2

    def serve_to(start, stop):
        if stop > start:
            lax.fori_loop(start, stop, lambda s, carry: (service(s), carry)[1], 0)

    low = z < chips // 2

    def grads_of(k, carry):
        chip = jnp.where(low, k, chips - 1 - k)
        for q in range(CHUNKS):
            to_partner(chip, q).wait_recv()
        rows = rows_at(chip * 2 * block, 2 * block)
        back = lax.dot_general(
            dall[rows, :], w_v[...], (((1,), (1,)), ((), ())), preferred_element_type=f32
        )
        g = gate_grad[rows, :].astype(f32)
        u = up_grad[rows, :].astype(f32)
        sig = jax.nn.sigmoid(g)
        gate_grad[rows, :] = (back * u * sig * (1.0 + g * (1.0 - sig))).astype(bf16)
        up_grad[rows, :] = (back * (g * sig)).astype(bf16)
        return carry

    serve_to(served, 2 * CHUNKS)
    lax.fori_loop(0, chips // 2, grads_of, 0)
    serve_to(max(served, 2 * CHUNKS), (chips - 1) * CHUNKS)
    lax.fori_loop(chips // 2, chips, grads_of, 0)

    wide = 256
    last = (chips - 1) * CHUNKS
    loads[6].wait()
    service(last)
    finish(0)

    def make_weight(i, carry):
        here = rows_at(i * wide, wide)
        weight_grad[:, here] = jnp.dot(
            hidden_t[...], dall[:, here], preferred_element_type=f32
        ).astype(bf16)
        return carry

    turns = model // wide
    marks = [turns * k // (CHUNKS - 1) for k in range(CHUNKS)]
    for q in range(1, CHUNKS):
        lax.fori_loop(marks[q - 1], marks[q], make_weight, 0)
        service(last + q)
        finish(q)

    for chip in range(chips):
        for q in range(CHUNKS):
            to_partner(chip, q).wait_send()
    for step in range(1, replicas):
        for copy in comp_copies(step):
            copy.wait_send()
    for way in range(2):
        @pl.when(onward[way])
        def _():
            for s in range(chips * CHUNKS):
                send(way, s, grad_piece(z, 0), grad_piece(z, 0)).wait_send()


def joint_scratch(n, replicas, tokens, units, model, span_rows, listed):
    chips, block = n // 2, tokens // n
    bf16, f32 = jnp.bfloat16, jnp.float32
    dma = pltpu.SemaphoreType.DMA
    arrays = [
        ((tokens, model), bf16),
        (((chips - 1) * block, model), bf16),
        (((chips - 1) * block, model), bf16),
        ((chips * block, model), bf16),
        ((units, model), bf16),
        ((tokens, units), bf16),
        ((units, tokens), bf16),
        ((replicas, span_rows, 1, listed), jnp.int32),
        ((replicas, span_rows, listed), bf16),
        ((span_rows, replicas, listed), jnp.int32),
        ((span_rows, replicas, listed), f32),
        ((listed // LANES * SPAN, LANES // TOPK * SPAN), bf16),
        ((block // CHUNKS, model), f32),
    ]
    total = sum(int(np.prod(shape)) * jnp.dtype(kind).itemsize for shape, kind in arrays)
    steps = chips * CHUNKS
    sems = [
        dma((7,)), dma((2, replicas - 1)), dma((2, replicas - 1)), dma((2, steps)), dma((2, steps)),
        dma((steps,)), dma((steps,)), dma((chips,)), dma((chips,)),
    ]
    return total, [pltpu.VMEM(shape, kind) for shape, kind in arrays] + sems


def joint(residual_r, gate_r, up_r, down_weight, grads_r, index_r, value_r, scratch):
    n, replicas = lax.axis_size("tp"), lax.axis_size("rep")
    (tokens, units), model = gate_r.shape, down_weight.shape[1]
    right, left = decode_tables()
    any_spec = pl.BlockSpec(memory_space=pl.ANY)
    vmem_spec = pl.BlockSpec(memory_space=pltpu.VMEM)
    shapes = [residual_r.shape, (tokens, units), (tokens, units)] + [(units, model)] * 3
    kept = pl.pallas_call(
        functools.partial(joint_kernel, n, replicas),
        out_shape=[pltpu.VMEM(shape, jnp.bfloat16) for shape in shapes],
        in_specs=[any_spec] * 7 + [vmem_spec] * 2,
        out_specs=[vmem_spec] * 6,
        scratch_shapes=scratch,
        compiler_params=pltpu.CompilerParams(
            collective_id=0, has_side_effects=True, vmem_limit_bytes=VMEM_BYTES
        ),
        cost_estimate=pl.CostEstimate(
            flops=6 * tokens * units * model, bytes_accessed=units * model * 8, transcendentals=0
        ),
        name="joint",
    )(residual_r, gate_r, up_r, down_weight, grads_r, index_r[:, None], value_r, right, left)
    return pl.pallas_call(
        put_kernel,
        out_shape=[jax.ShapeDtypeStruct(shape, jnp.bfloat16) for shape in shapes],
        in_specs=[vmem_spec] * 6,
        out_specs=[any_spec] * 6,
        scratch_shapes=[pltpu.SemaphoreType.DMA((6,))],
        compiler_params=pltpu.CompilerParams(vmem_limit_bytes=PUT_BYTES),
        name="put",
    )(*kept)


def put_kernel(*refs):
    sem = refs[-1]
    copies = [pltpu.make_async_copy(refs[i], refs[6 + i], sem.at[i]) for i in range(6)]
    for copy in copies:
        copy.start()
    for copy in copies:
        copy.wait()


def chips_rows(n, tokens):
    return n // 2 * (tokens // n)


def shards(residual, gate_pre, up_pre, down_weight, d_out, comp_index, comp_value):
    operands = (residual[0], gate_pre[0], up_pre[0], down_weight, d_out[0], comp_index[0], comp_value[0])
    n, replicas = lax.axis_size("tp"), lax.axis_size("rep")
    tokens, units = gate_pre.shape[1:]
    span_rows, listed = comp_index.shape[1:]
    model = down_weight.shape[1]
    fits = False
    if n % 4 == 0 and units % LANES == 0 and span_rows % 2 == 0 and replicas % 2 == 0:
        total, scratch = joint_scratch(n, replicas, tokens, units, model, span_rows, listed)
        fits = total < 36 * 2**20 and units >= chips_rows(n, tokens) and n // 2 == CHUNKS
    if fits:
        outs = joint(*operands, scratch)
    else:
        outs = plain_shards(*operands)
    output, gate_preact_gradient, up_grad, weight_sum, update, updated = outs
    return (
        output[None],
        gate_preact_gradient[None],
        up_grad[None],
        weight_sum[None],
        update,
        updated,
    )


def solution(mesh):
    return jax.shard_map(
        shards,
        mesh=mesh,
        in_specs=(
            P("rep", "tp", None),
            P("rep", None, "tp"),
            P("rep", None, "tp"),
            P("tp", None),
            P("rep", "tp", None),
            P("rep", "tp", None),
            P("rep", "tp", None),
        ),
        out_specs=(
            P("rep", "tp", None),
            P("rep", None, "tp"),
            P("rep", None, "tp"),
            P("rep", "tp", None),
            P("tp", None),
            P("tp", None),
        ),
        check_vma=False,
    )
```

```python
import functools

import jax
import jax.numpy as jnp
import numpy as np
from jax import lax
from jax.experimental import pallas as pl
from jax.experimental.pallas import tpu as pltpu
from jax.sharding import PartitionSpec as P

SPAN = 64
TOPK = 32


learn_rate = 0.02


LANES = 128
UNROLL = 4
MESH = pl.DeviceIdType.MESH
VMEM_BYTES = 38 * 2**20
PUT_BYTES = 2**20
CHUNKS = 4
FIRST = 2


def cosine_table(length):
    freq = np.arange(length, dtype=np.float64)[:, None]
    place = np.arange(length, dtype=np.float64)[None, :]
    scales = np.where(freq == 0, np.sqrt(1.0 / length), np.sqrt(2.0 / length))
    return scales * np.cos(np.pi * (2.0 * place + 1.0) * freq / (2.0 * length))


def decode_kernel(count, *refs):
    index_refs, value_refs = refs[:count], refs[count:2 * count]
    weight_ref, right_ref, left_ref, update_ref, weight_out_ref, mixed_ref = refs[2 * count:]
    groups = index_refs[0].shape[1] // LANES
    per_group = LANES // TOPK
    width = per_group * SPAN
    depth = count * LANES
    lane = lax.broadcasted_iota(jnp.int32, (1, depth), 1)
    shift = ((lane // TOPK) % per_group) * SPAN
    row_place = lax.broadcasted_iota(jnp.int32, (SPAN, depth), 0).astype(jnp.float32).astype(jnp.bfloat16)
    col_place = lax.broadcasted_iota(jnp.int32, (width, depth), 0).astype(jnp.float32).astype(jnp.bfloat16)

    def gather(group, carry):
        at = pl.ds(pl.multiple_of(group * LANES, LANES), LANES)
        words = jnp.concatenate([ref[:, at] for ref in index_refs], axis=1)
        values = jnp.concatenate([ref[:, at] for ref in value_refs], axis=1).astype(jnp.bfloat16)
        rows = (words >> (SPAN.bit_length() - 1)).astype(jnp.float32).astype(jnp.bfloat16)
        cols = ((words & (SPAN - 1)) + shift).astype(jnp.float32).astype(jnp.bfloat16)
        row_hot = jnp.where(rows == row_place, values, jnp.bfloat16(0))
        col_hot = jnp.where(cols == col_place, jnp.bfloat16(1), jnp.bfloat16(0))
        spectral = lax.dot_general(
            row_hot, col_hot, (((1,), (1,)), ((), ())), preferred_element_type=jnp.float32
        )
        mixed_ref[pl.ds(pl.multiple_of(group * SPAN, SPAN), SPAN), :] = spectral.astype(jnp.bfloat16)
        return carry

    lax.fori_loop(0, groups, gather, 0, unroll=UNROLL)
    halfway = jnp.dot(
        mixed_ref[...], right_ref[...], preferred_element_type=jnp.float32
    ).astype(jnp.bfloat16)
    for group in range(groups):
        block = jnp.dot(
            left_ref[...], halfway[group * SPAN:(group + 1) * SPAN], preferred_element_type=jnp.float32
        )
        change = (block * (1.0 / count)).astype(jnp.bfloat16)
        at = slice(group * width, (group + 1) * width)
        update_ref[:, at] = change
        weight_out_ref[:, at] = (
            weight_ref[:, at].astype(jnp.float32) - learn_rate * change.astype(jnp.float32)
        ).astype(jnp.bfloat16)


def decode_tables():
    basis = cosine_table(SPAN)
    right = jnp.asarray(np.kron(np.eye(LANES // TOPK), basis), jnp.bfloat16)
    left = jnp.asarray(basis.T, jnp.bfloat16)
    return right, left


def decode(indices, values, down_weight):
    count = len(indices)
    span_rows, _, listed = indices[0].shape
    units, model = down_weight.shape
    per_group = LANES // TOPK
    width = per_group * SPAN
    right, left = decode_tables()
    strip = pl.BlockSpec((SPAN, model), lambda a: (a, 0))
    whole = lambda shape: pl.BlockSpec(shape, lambda a: (0, 0))
    return pl.pallas_call(
        functools.partial(decode_kernel, count),
        grid=(span_rows,),
        out_shape=[jax.ShapeDtypeStruct((units, model), jnp.bfloat16)] * 2,
        in_specs=[pl.BlockSpec((None, 1, listed), lambda a: (a, 0, 0))] * (2 * count)
        + [strip, whole((width, width)), whole((SPAN, SPAN))],
        out_specs=[strip, strip],
        scratch_shapes=[pltpu.VMEM((listed // LANES * SPAN, width), jnp.bfloat16)],
        compiler_params=pltpu.CompilerParams(
            dimension_semantics=("arbitrary",), vmem_limit_bytes=24 * 2**20
        ),
        cost_estimate=pl.CostEstimate(
            flops=20 * 10**9, bytes_accessed=units * model * 6, transcendentals=0
        ),
        name="decode",
    )(*indices, *values, down_weight, right, left)


def plain_shards(residual_r, gate_r, up_r, down_weight, grads_r, index_r, value_r):
    replicas = lax.axis_size("rep")

    def from_replicas(mine):
        return [mine] + [
            lax.ppermute(mine, "rep", [(i, (i + step) % replicas) for i in range(replicas)])
            for step in range(1, replicas)
        ]

    indices = from_replicas(index_r[:, None])
    values = from_replicas(value_r.astype(jnp.float32)[:, None])
    gate_f = gate_r.astype(jnp.float32)
    up_f = up_r.astype(jnp.float32)
    sigmoid_g = jax.nn.sigmoid(gate_f)
    activated = gate_f * sigmoid_g
    hidden = (activated * up_f).astype(jnp.bfloat16)
    summed = lax.psum_scatter(
        jnp.dot(hidden, down_weight, preferred_element_type=jnp.float32).astype(jnp.bfloat16),
        "tp",
        scatter_dimension=0,
        tiled=True,
    ).astype(jnp.float32)
    incoming = lax.all_gather(grads_r, "tp", axis=0, tiled=True)
    hidden_grad = lax.dot_general(
        incoming, down_weight, (((1,), (1,)), ((), ())), preferred_element_type=jnp.float32
    )
    weight_sum = lax.dot_general(
        hidden, incoming, (((0,), (0,)), ((), ())), preferred_element_type=jnp.float32
    )
    output = (residual_r.astype(jnp.float32) + summed).astype(jnp.bfloat16)
    gate_preact_gradient = (
        hidden_grad * up_f * sigmoid_g * (1.0 + gate_f * (1.0 - sigmoid_g))
    ).astype(jnp.bfloat16)
    up_grad = (hidden_grad * activated).astype(jnp.bfloat16)
    update, updated_down_weight = decode(indices, values, down_weight)
    return output, gate_preact_gradient, up_grad, weight_sum.astype(jnp.bfloat16), update, updated_down_weight


def rows_at(start, size):
    return pl.ds(pl.multiple_of(start, size), size)


def joint_kernel(
    n, replicas,
    residual, gate, up, weight, grads, index, value, right_ref, left_ref,
    output, gate_grad, up_grad, weight_grad, update, updated, late,
    dall, slot_up, slot_dn, part, w_v, hidden, hidden_t,
    index_v, value_v, word_v, amount_v, mixed, fin,
    load_sem, comp_send, comp_recv, step_send, step_recv, chip_send, chip_recv,
    part_send, part_recv, late_sem,
):
    chips = n // 2
    rep = lax.axis_index("rep")
    me = lax.axis_index("tp")
    z, core = me // 2, me % 2
    partner = me + 1 - 2 * core
    tokens, units = gate_grad.shape
    model = w_v.shape[1]
    block = tokens // n
    piece = block // CHUNKS
    span_rows, listed = value_v.shape[1], value_v.shape[2]
    groups = listed // LANES
    per_group = LANES // TOPK
    width = per_group * SPAN
    f32, bf16 = jnp.float32, jnp.bfloat16

    loads = [
        pltpu.make_async_copy(gate, gate_grad, load_sem.at[0]),
        pltpu.make_async_copy(up, up_grad, load_sem.at[1]),
        pltpu.make_async_copy(weight, w_v, load_sem.at[2]),
        pltpu.make_async_copy(grads, dall.at[rows_at(me * block, block)], load_sem.at[3]),
        pltpu.make_async_copy(index, index_v.at[rep], load_sem.at[4]),
        pltpu.make_async_copy(value, value_v.at[rep], load_sem.at[5]),
        pltpu.make_async_copy(residual, output, load_sem.at[6]),
    ]
    for load in loads:
        load.start()

    barrier = pltpu.get_barrier_semaphore()
    has_up, has_dn = z < chips - 1, z > 0

    @pl.when(has_up)
    def _():
        pl.semaphore_signal(barrier, inc=1, device_id={"tp": me + 2}, device_id_type=MESH)

    @pl.when(has_dn)
    def _():
        pl.semaphore_signal(barrier, inc=1, device_id={"tp": me - 2}, device_id_type=MESH)

    pl.semaphore_signal(barrier, inc=1, device_id={"tp": partner}, device_id_type=MESH)
    for step in range(1, replicas):
        pl.semaphore_signal(
            barrier, inc=1, device_id={"rep": (rep + step) % replicas}, device_id_type=MESH
        )
    pl.semaphore_wait(barrier, replicas + has_up.astype(jnp.int32) + has_dn.astype(jnp.int32))

    def send(way, s, src, dst):
        return pltpu.make_async_remote_copy(
            src_ref=src, dst_ref=dst, send_sem=step_send.at[way, s], recv_sem=step_recv.at[way, s],
            device_id={"tp": me + (2 if way == 0 else -2)}, device_id_type=MESH,
        )

    def grad_piece(chip, q):
        return dall.at[rows_at((2 * chip + core) * block + q * piece, piece)]

    def to_partner(chip, q):
        return pltpu.make_async_remote_copy(
            src_ref=grad_piece(chip, q), dst_ref=grad_piece(chip, q),
            send_sem=chip_send.at[chip * CHUNKS + q], recv_sem=chip_recv.at[chip * CHUNKS + q],
            device_id={"tp": partner}, device_id_type=MESH,
        )

    lent = units - chips * block

    def hand_over(target):
        return pltpu.make_async_remote_copy(
            src_ref=update.at[pl.ds(lent + target * block, block)],
            dst_ref=weight_grad.at[pl.ds(target * block, block)],
            send_sem=part_send.at[target], recv_sem=part_recv.at[target],
            device_id={"tp": partner}, device_id_type=MESH,
        )

    def comp_copies(step):
        to = {"rep": (rep + step) % replicas}
        return [
            pltpu.make_async_remote_copy(
                src_ref=src, dst_ref=dst.at[rep], send_sem=comp_send.at[kind, step - 1],
                recv_sem=comp_recv.at[kind, step - 1], device_id=to, device_id_type=MESH,
            )
            for kind, (src, dst) in enumerate(((index, index_v), (value, value_v)))
        ]

    slots = (slot_up, slot_dn)
    rank = (z, chips - 1 - z)
    onward = (has_up, has_dn)
    behind = (has_dn, has_up)

    for q in range(CHUNKS):
        for way in range(2):
            @pl.when(onward[way])
            def _():
                send(way, q, grads.at[pl.ds(q * piece, piece)], grad_piece(z, q)).start()

    for step in range(1, replicas):
        for copy in comp_copies(step):
            copy.start()

    loads[3].wait()
    for q in range(CHUNKS):
        to_partner(z, q).start()

    def own_sum(target, q):
        return part[rows_at(target * block + q * piece, piece), :]

    def slot_rows(p, q):
        return rows_at((p - 1) * block + q * piece, piece)

    def put_late(source, q):
        return pltpu.make_async_copy(source, late.at[rows_at(q * piece, piece)], late_sem.at[q])

    def service(s):
        p, q = s // CHUNKS, s % CHUNKS
        for way in range(2):
            at, slot = rank[way], slots[way]
            gathered = p < at
            source = z - 1 - p if way == 0 else z + 1 + p
            target = chips + z - 1 - p if way == 0 else z - chips + 1 + p
            summing = jnp.logical_and(jnp.logical_and(p >= at, onward[way]), p < chips - 1)
            first = at == 0

            def pass_on(source):
                after = jnp.logical_and(p == chips - 2, core == way)

                @pl.when(after)
                def _():
                    put_late(source, q).start()

                @pl.when(jnp.logical_not(after))
                def _():
                    send(way, s + CHUNKS, source, slot.at[slot_rows(p + 1, q)]).start()

            @pl.when(jnp.logical_and(behind[way], jnp.logical_or(p < chips - 1, core != way)))
            def _():
                send(way, s, grad_piece(z, q), grad_piece(z, q)).wait_recv()

            @pl.when(gathered)
            def _():
                to_partner(source, q).start()

                @pl.when(onward[way])
                def _():
                    send(way, s + CHUNKS, grad_piece(source, q), grad_piece(source, q)).start()

            @pl.when(jnp.logical_and(summing, first))
            def _():
                pass_on(part.at[rows_at(target * block + q * piece, piece)])

            @pl.when(jnp.logical_and(summing, jnp.logical_not(first)))
            def _():
                here = slot_rows(p, q)
                slot[here, :] = (own_sum(target, q).astype(f32) + slot[here, :].astype(f32)).astype(bf16)
                pass_on(slot.at[here])

    def finish(q):
        here = rows_at(q * piece, piece)
        fin[...] = output[here, :].astype(f32) + own_sum(z, q).astype(f32)
        for way in range(2):
            @pl.when(jnp.logical_and(behind[way], core != way))
            def _():
                fin[...] = fin[...] + slots[way][rows_at((chips - 2) * block + q * piece, piece), :].astype(f32)
        output[here, :] = fin[...].astype(bf16)

    loads[0].wait()
    loads[1].wait()

    def make_hidden(i, carry):
        here = rows_at(i * block, block)
        g = gate_grad[here, :].astype(f32)
        u = up_grad[here, :].astype(f32)
        h = (g * jax.nn.sigmoid(g) * u).astype(bf16)
        hidden[here, :] = h
        hidden_t[:, here] = h.astype(f32).T.astype(bf16)
        return carry

    tile = 512

    def target_at(k):
        return jnp.where(k % 2 == 0, chips - 1 - k // 2, k // 2)

    def add_other(k):
        target = target_at(k)
        hand_over(target).wait_recv()

        def add_part(q, carry):
            here = rows_at(target * block + q * piece, piece)
            part[here, :] = (part[here, :].astype(f32) + weight_grad[here, :].astype(f32)).astype(bf16)
            return carry

        lax.fori_loop(0, CHUNKS, add_part, 0)

    def make_target(k, carry):
        target = target_at(k)
        lax.fori_loop(2 * target, 2 * target + 2, make_hidden, 0)
        rows = rows_at(2 * target * block, 2 * block)
        mine, other = rows_at(target * block, block), rows_at(lent + target * block, block)

        def make_part(i, carry):
            here = rows_at(i * tile, tile)
            got = jnp.dot(hidden[rows, :], w_v[:, here], preferred_element_type=f32).astype(bf16)

            @pl.when(core == 0)
            def _():
                part[mine, here] = got[:block]
                update[other, here] = got[block:]

            @pl.when(core == 1)
            def _():
                part[mine, here] = got[block:]
                update[other, here] = got[:block]
            return carry

        lax.fori_loop(0, model // tile, make_part, 0)
        hand_over(target).start()

        @pl.when(k > 0)
        def _():
            add_other(k - 1)

        @pl.when(k >= FIRST)
        def _():
            service(k - FIRST)

        return carry

    loads[2].wait()
    lax.fori_loop(0, chips, make_target, 0)

    for step in range(1, replicas):
        for copy in comp_copies(step):
            copy.wait_recv()
    loads[4].wait()
    loads[5].wait()

    pairs = replicas // 2
    half = LANES // 2
    spot = lax.broadcasted_iota(jnp.int32, (1, listed), 1)
    lower = spot % LANES < half
    for a in range(span_rows):
        for j in range(pairs):
            for dest, pick in (
                (word_v, lambda r: index_v[r, a]),
                (amount_v, lambda r: value_v[r].astype(f32)[a:a + 1]),
            ):
                even, odd = pick(2 * j), pick(2 * j + 1)
                dest[a, j:j + 1, :] = jnp.where(lower, even, pltpu.roll(odd, half, 1))
                dest[a, pairs + j:pairs + j + 1, :] = jnp.where(lower, pltpu.roll(even, listed - half, 1), odd)

    deep = pairs * LANES
    shift = ((lax.broadcasted_iota(jnp.int32, (replicas, LANES), 1) // TOPK) % 2) * SPAN
    row_place = lax.broadcasted_iota(jnp.int32, (SPAN, deep), 0).astype(f32).astype(bf16)
    col_place = lax.broadcasted_iota(jnp.int32, (2 * SPAN, deep), 0).astype(f32).astype(bf16)

    def decode_row(a):
        def gather(group, carry):
            at = rows_at(group * LANES, LANES)
            words = word_v[a, :, at]
            row_set = (words >> (SPAN.bit_length() - 1)).astype(f32)
            col_set = ((words & (SPAN - 1)) + shift).astype(f32)
            amount_set = amount_v[a, :, at]
            for side in range(2):
                line = lambda x: jnp.concatenate(
                    [x[side * pairs + j:side * pairs + j + 1] for j in range(pairs)], axis=1
                ).astype(bf16)
                row_hot = jnp.where(line(row_set) == row_place, line(amount_set), bf16(0))
                col_hot = jnp.where(line(col_set) == col_place, bf16(1), bf16(0))
                spectral = lax.dot_general(
                    row_hot, col_hot, (((1,), (1,)), ((), ())), preferred_element_type=f32
                )
                mixed[rows_at(group * SPAN, SPAN), side * 2 * SPAN:(side + 1) * 2 * SPAN] = spectral.astype(bf16)
            return carry

        lax.fori_loop(0, groups, gather, 0, unroll=UNROLL)
        halfway = jnp.dot(mixed[...], right_ref[...], preferred_element_type=f32).astype(bf16)
        rows = rows_at(a * SPAN, SPAN)
        for group in range(groups):
            spread = jnp.dot(
                left_ref[...], halfway[group * SPAN:(group + 1) * SPAN], preferred_element_type=f32
            )
            change = (spread * (1.0 / replicas)).astype(bf16)
            at = slice(group * width, (group + 1) * width)
            update[rows, at] = change
            updated[rows, at] = (w_v[rows, at].astype(f32) - learn_rate * change.astype(f32)).astype(bf16)

    def decode_step(a, carry):
        decode_row(a)

        @pl.when(a % 3 == 2)
        def _():
            service(chips - FIRST + a // 3)

        return carry

    add_other(chips - 1)
    for target in range(chips):
        hand_over(target).wait_send()
    lax.fori_loop(0, span_rows, decode_step, 0)
    served = chips - FIRST + span_rows // 3

    low = z < chips // 2

    def grads_of(k, carry):
        chip = jnp.where(low, k, chips - 1 - k)
        for q in range(CHUNKS):
            to_partner(chip, q).wait_recv()
        rows = rows_at(chip * 2 * block, 2 * block)
        back = lax.dot_general(
            dall[rows, :], w_v[...], (((1,), (1,)), ((), ())), preferred_element_type=f32
        )
        g = gate_grad[rows, :].astype(f32)
        u = up_grad[rows, :].astype(f32)
        sig = jax.nn.sigmoid(g)
        gate_grad[rows, :] = (back * u * sig * (1.0 + g * (1.0 - sig))).astype(bf16)
        up_grad[rows, :] = (back * (g * sig)).astype(bf16)
        return carry

    def serve_loop(start, stop):
        lax.fori_loop(start, stop, lambda s, carry: (service(s), carry)[1], 0)

    def grads_early(k, carry):
        grads_of(k, carry)

        @pl.when(served + k < 2 * CHUNKS)
        def _():
            service(served + k)

        return carry

    wide = 256
    turns = model // wide
    last = (chips - 1) * CHUNKS
    near = 2 * block * (chips - 1)
    near_at = jnp.where(low, 0, 2 * block)
    far_at = jnp.where(low, near, 0)
    between = CHUNKS - 1

    def weight_near(i, carry):
        here = rows_at(i * wide, wide)
        rows = pl.ds(pl.multiple_of(near_at, 2 * block), near)
        weight_grad[:, here] = jnp.dot(
            hidden_t[:, rows], dall[rows, here], preferred_element_type=f32
        ).astype(bf16)

        @pl.when(i % (turns // between) == turns // between - 1)
        def _():
            service(2 * CHUNKS + i // (turns // between))

        return carry

    def weight_far(i, carry):
        here = rows_at(i * wide, wide)
        rows = rows_at(far_at, 2 * block)
        more = jnp.dot(hidden_t[:, rows], dall[rows, here], preferred_element_type=f32)
        weight_grad[:, here] = (weight_grad[:, here].astype(f32) + more).astype(bf16)

        @pl.when(i % (turns // CHUNKS) == turns // CHUNKS - 1)
        def _():
            service(last + i // (turns // CHUNKS))
            finish(i // (turns // CHUNKS))

        return carry

    lax.fori_loop(0, chips - 2, grads_early, 0)
    serve_loop(served + chips - 2, 2 * CHUNKS)
    grads_of(chips - 2, 0)
    lax.fori_loop(0, turns, weight_near, 0)
    service(last - 1)
    grads_of(chips - 1, 0)
    loads[6].wait()
    lax.fori_loop(0, turns, weight_far, 0)

    for chip in range(chips):
        for q in range(CHUNKS):
            to_partner(chip, q).wait_send()
    for step in range(1, replicas):
        for copy in comp_copies(step):
            copy.wait_send()
    for way in range(2):
        @pl.when(onward[way])
        def _():
            for s in range(last):
                send(way, s, grad_piece(z, 0), grad_piece(z, 0)).wait_send()

            @pl.when(core != way)
            def _():
                for s in range(last, last + CHUNKS):
                    send(way, s, grad_piece(z, 0), grad_piece(z, 0)).wait_send()

            @pl.when(core == way)
            def _():
                for q in range(CHUNKS):
                    put_late(part.at[pl.ds(0, piece)], q).wait()


def joint_scratch(n, replicas, tokens, units, model, span_rows, listed):
    chips, block = n // 2, tokens // n
    bf16, f32 = jnp.bfloat16, jnp.float32
    dma = pltpu.SemaphoreType.DMA
    arrays = [
        ((tokens, model), bf16),
        (((chips - 1) * block, model), bf16),
        (((chips - 1) * block, model), bf16),
        ((chips * block, model), bf16),
        ((units, model), bf16),
        ((tokens, units), bf16),
        ((units, tokens), bf16),
        ((replicas, span_rows, 1, listed), jnp.int32),
        ((replicas, span_rows, listed), bf16),
        ((span_rows, replicas, listed), jnp.int32),
        ((span_rows, replicas, listed), f32),
        ((listed // LANES * SPAN, LANES // TOPK * SPAN), bf16),
        ((block // CHUNKS, model), f32),
    ]
    total = sum(int(np.prod(shape)) * jnp.dtype(kind).itemsize for shape, kind in arrays)
    steps = chips * CHUNKS
    sems = [
        dma((7,)), dma((2, replicas - 1)), dma((2, replicas - 1)), dma((2, steps)), dma((2, steps)),
        dma((steps,)), dma((steps,)), dma((chips,)), dma((chips,)), dma((CHUNKS,)),
    ]
    return total, [pltpu.VMEM(shape, kind) for shape, kind in arrays] + sems


def joint(residual_r, gate_r, up_r, down_weight, grads_r, index_r, value_r, scratch):
    n, replicas = lax.axis_size("tp"), lax.axis_size("rep")
    (tokens, units), model = gate_r.shape, down_weight.shape[1]
    right, left = decode_tables()
    any_spec = pl.BlockSpec(memory_space=pl.ANY)
    vmem_spec = pl.BlockSpec(memory_space=pltpu.VMEM)
    shapes = [residual_r.shape, (tokens, units), (tokens, units)] + [(units, model)] * 3
    *kept, late = pl.pallas_call(
        functools.partial(joint_kernel, n, replicas),
        out_shape=[pltpu.VMEM(shape, jnp.bfloat16) for shape in shapes]
        + [jax.ShapeDtypeStruct(residual_r.shape, jnp.bfloat16)],
        in_specs=[any_spec] * 7 + [vmem_spec] * 2,
        out_specs=[vmem_spec] * 6 + [any_spec],
        scratch_shapes=scratch,
        compiler_params=pltpu.CompilerParams(
            collective_id=0, has_side_effects=True, vmem_limit_bytes=VMEM_BYTES
        ),
        cost_estimate=pl.CostEstimate(
            flops=6 * tokens * units * model, bytes_accessed=units * model * 8, transcendentals=0
        ),
        name="joint",
    )(residual_r, gate_r, up_r, down_weight, grads_r, index_r[:, None], value_r, right, left)
    hops = [(i, i + 2) for i in range(0, n - 2, 2)] + [(i, i - 2) for i in range(3, n, 2)]
    arrived = lax.ppermute(late, "tp", hops)
    early, *kept = kept
    placed = pl.pallas_call(
        put_kernel,
        out_shape=[jax.ShapeDtypeStruct(shape, jnp.bfloat16) for shape in shapes[1:]],
        in_specs=[vmem_spec] * 5,
        out_specs=[any_spec] * 5,
        scratch_shapes=[pltpu.SemaphoreType.DMA((5,))],
        compiler_params=pltpu.CompilerParams(vmem_limit_bytes=PUT_BYTES),
        cost_estimate=pl.CostEstimate(
            flops=2 * tokens * units * model, bytes_accessed=units * model * 8, transcendentals=0
        ),
        name="put",
    )(*kept)
    output = (early.astype(jnp.float32) + arrived.astype(jnp.float32)).astype(jnp.bfloat16)
    return [output] + list(placed)


def put_kernel(*refs):
    sem = refs[-1]
    count = len(refs) // 2
    copies = [pltpu.make_async_copy(refs[i], refs[count + i], sem.at[i]) for i in range(count)]
    for copy in copies:
        copy.start()
    for copy in copies:
        copy.wait()


def chips_rows(n, tokens):
    return n // 2 * (tokens // n)


def shards(residual, gate_pre, up_pre, down_weight, d_out, comp_index, comp_value):
    operands = (residual[0], gate_pre[0], up_pre[0], down_weight, d_out[0], comp_index[0], comp_value[0])
    n, replicas = lax.axis_size("tp"), lax.axis_size("rep")
    tokens, units = gate_pre.shape[1:]
    span_rows, listed = comp_index.shape[1:]
    model = down_weight.shape[1]
    fits = False
    if n % 4 == 0 and units % LANES == 0 and span_rows % 2 == 0 and replicas % 2 == 0:
        total, scratch = joint_scratch(n, replicas, tokens, units, model, span_rows, listed)
        fits = total < 36 * 2**20 and units >= chips_rows(n, tokens) and n // 2 == CHUNKS and 2 * CHUNKS >= CHUNKS - FIRST + span_rows // 3 + 2
    if fits:
        outs = joint(*operands, scratch)
    else:
        outs = plain_shards(*operands)
    output, gate_preact_gradient, up_grad, weight_sum, update, updated = outs
    return (
        output[None],
        gate_preact_gradient[None],
        up_grad[None],
        weight_sum[None],
        update,
        updated,
    )


def solution(mesh):
    return jax.shard_map(
        shards,
        mesh=mesh,
        in_specs=(
            P("rep", "tp", None),
            P("rep", None, "tp"),
            P("rep", None, "tp"),
            P("tp", None),
            P("rep", "tp", None),
            P("rep", "tp", None),
            P("rep", "tp", None),
        ),
        out_specs=(
            P("rep", "tp", None),
            P("rep", None, "tp"),
            P("rep", None, "tp"),
            P("rep", "tp", None),
            P("tp", None),
            P("tp", None),
        ),
        check_vma=False,
    )
```

```python
import functools

import jax
import jax.numpy as jnp
import numpy as np
from jax import lax
from jax.experimental import pallas as pl
from jax.experimental.pallas import tpu as pltpu
from jax.sharding import PartitionSpec as P

SPAN = 64
TOPK = 32


learn_rate = 0.02


LANES = 128
UNROLL = 4
MESH = pl.DeviceIdType.MESH
VMEM_BYTES = 38 * 2**20
PUT_BYTES = 2**20
PUT_PARTS = 4
CHUNKS = 4
FIRST = 2


def cosine_table(length):
    freq = np.arange(length, dtype=np.float64)[:, None]
    place = np.arange(length, dtype=np.float64)[None, :]
    scales = np.where(freq == 0, np.sqrt(1.0 / length), np.sqrt(2.0 / length))
    return scales * np.cos(np.pi * (2.0 * place + 1.0) * freq / (2.0 * length))


def decode_kernel(count, *refs):
    index_refs, value_refs = refs[:count], refs[count:2 * count]
    weight_ref, right_ref, left_ref, update_ref, weight_out_ref, mixed_ref = refs[2 * count:]
    groups = index_refs[0].shape[1] // LANES
    per_group = LANES // TOPK
    width = per_group * SPAN
    depth = count * LANES
    lane = lax.broadcasted_iota(jnp.int32, (1, depth), 1)
    shift = ((lane // TOPK) % per_group) * SPAN
    row_place = lax.broadcasted_iota(jnp.int32, (SPAN, depth), 0).astype(jnp.float32).astype(jnp.bfloat16)
    col_place = lax.broadcasted_iota(jnp.int32, (width, depth), 0).astype(jnp.float32).astype(jnp.bfloat16)

    def gather(group, carry):
        at = pl.ds(pl.multiple_of(group * LANES, LANES), LANES)
        words = jnp.concatenate([ref[:, at] for ref in index_refs], axis=1)
        values = jnp.concatenate([ref[:, at] for ref in value_refs], axis=1).astype(jnp.bfloat16)
        rows = (words >> (SPAN.bit_length() - 1)).astype(jnp.float32).astype(jnp.bfloat16)
        cols = ((words & (SPAN - 1)) + shift).astype(jnp.float32).astype(jnp.bfloat16)
        row_hot = jnp.where(rows == row_place, values, jnp.bfloat16(0))
        col_hot = jnp.where(cols == col_place, jnp.bfloat16(1), jnp.bfloat16(0))
        spectral = lax.dot_general(
            row_hot, col_hot, (((1,), (1,)), ((), ())), preferred_element_type=jnp.float32
        )
        mixed_ref[pl.ds(pl.multiple_of(group * SPAN, SPAN), SPAN), :] = spectral.astype(jnp.bfloat16)
        return carry

    lax.fori_loop(0, groups, gather, 0, unroll=UNROLL)
    halfway = jnp.dot(
        mixed_ref[...], right_ref[...], preferred_element_type=jnp.float32
    ).astype(jnp.bfloat16)
    for group in range(groups):
        block = jnp.dot(
            left_ref[...], halfway[group * SPAN:(group + 1) * SPAN], preferred_element_type=jnp.float32
        )
        change = (block * (1.0 / count)).astype(jnp.bfloat16)
        at = slice(group * width, (group + 1) * width)
        update_ref[:, at] = change
        weight_out_ref[:, at] = (
            weight_ref[:, at].astype(jnp.float32) - learn_rate * change.astype(jnp.float32)
        ).astype(jnp.bfloat16)


def decode_tables():
    basis = cosine_table(SPAN)
    right = jnp.asarray(np.kron(np.eye(LANES // TOPK), basis), jnp.bfloat16)
    left = jnp.asarray(basis.T, jnp.bfloat16)
    return right, left


def decode(indices, values, down_weight):
    count = len(indices)
    span_rows, _, listed = indices[0].shape
    units, model = down_weight.shape
    per_group = LANES // TOPK
    width = per_group * SPAN
    right, left = decode_tables()
    strip = pl.BlockSpec((SPAN, model), lambda a: (a, 0))
    whole = lambda shape: pl.BlockSpec(shape, lambda a: (0, 0))
    return pl.pallas_call(
        functools.partial(decode_kernel, count),
        grid=(span_rows,),
        out_shape=[jax.ShapeDtypeStruct((units, model), jnp.bfloat16)] * 2,
        in_specs=[pl.BlockSpec((None, 1, listed), lambda a: (a, 0, 0))] * (2 * count)
        + [strip, whole((width, width)), whole((SPAN, SPAN))],
        out_specs=[strip, strip],
        scratch_shapes=[pltpu.VMEM((listed // LANES * SPAN, width), jnp.bfloat16)],
        compiler_params=pltpu.CompilerParams(
            dimension_semantics=("arbitrary",), vmem_limit_bytes=24 * 2**20
        ),
        cost_estimate=pl.CostEstimate(
            flops=20 * 10**9, bytes_accessed=units * model * 6, transcendentals=0
        ),
        name="decode",
    )(*indices, *values, down_weight, right, left)


def plain_shards(residual_r, gate_r, up_r, down_weight, grads_r, index_r, value_r):
    replicas = lax.axis_size("rep")

    def from_replicas(mine):
        return [mine] + [
            lax.ppermute(mine, "rep", [(i, (i + step) % replicas) for i in range(replicas)])
            for step in range(1, replicas)
        ]

    indices = from_replicas(index_r[:, None])
    values = from_replicas(value_r.astype(jnp.float32)[:, None])
    gate_f = gate_r.astype(jnp.float32)
    up_f = up_r.astype(jnp.float32)
    sigmoid_g = jax.nn.sigmoid(gate_f)
    activated = gate_f * sigmoid_g
    hidden = (activated * up_f).astype(jnp.bfloat16)
    summed = lax.psum_scatter(
        jnp.dot(hidden, down_weight, preferred_element_type=jnp.float32).astype(jnp.bfloat16),
        "tp",
        scatter_dimension=0,
        tiled=True,
    ).astype(jnp.float32)
    incoming = lax.all_gather(grads_r, "tp", axis=0, tiled=True)
    hidden_grad = lax.dot_general(
        incoming, down_weight, (((1,), (1,)), ((), ())), preferred_element_type=jnp.float32
    )
    weight_sum = lax.dot_general(
        hidden, incoming, (((0,), (0,)), ((), ())), preferred_element_type=jnp.float32
    )
    output = (residual_r.astype(jnp.float32) + summed).astype(jnp.bfloat16)
    gate_preact_gradient = (
        hidden_grad * up_f * sigmoid_g * (1.0 + gate_f * (1.0 - sigmoid_g))
    ).astype(jnp.bfloat16)
    up_grad = (hidden_grad * activated).astype(jnp.bfloat16)
    update, updated_down_weight = decode(indices, values, down_weight)
    return output, gate_preact_gradient, up_grad, weight_sum.astype(jnp.bfloat16), update, updated_down_weight


def rows_at(start, size):
    return pl.ds(pl.multiple_of(start, size), size)


def flip(place, bits):
    for k in range(bits.bit_length()):
        if (bits >> k) & 1:
            place = place + (1 << k) * (1 - 2 * ((place // (1 << k)) % 2))
    return place


def joint_kernel(
    n, replicas,
    residual, gate, up, weight, grads, index, value, right, left,
    output, gate_grad, up_grad, weight_grad, update, updated, late,
    dall, slot_up, slot_dn, part, w_v, hidden, hidden_t,
    index_v, value_v, word_v, amount_v, mixed, fin, right_ref, left_ref,
    load_sem, comp_send, comp_recv, step_send, step_recv, chip_send, chip_recv,
    part_send, part_recv, late_sem,
):
    chips = n // 2
    rep = lax.axis_index("rep")
    me = lax.axis_index("tp")
    z, core = me // 2, me % 2
    partner = me + 1 - 2 * core
    tokens, units = gate_grad.shape
    model = w_v.shape[1]
    block = tokens // n
    piece = block // CHUNKS
    span_rows, listed = value_v.shape[1], value_v.shape[2]
    groups = listed // LANES
    per_group = LANES // TOPK
    width = per_group * SPAN
    f32, bf16 = jnp.float32, jnp.bfloat16

    loads = [
        pltpu.make_async_copy(gate, gate_grad, load_sem.at[0]),
        pltpu.make_async_copy(up, up_grad, load_sem.at[1]),
        pltpu.make_async_copy(weight, w_v, load_sem.at[2]),
        pltpu.make_async_copy(grads, dall.at[rows_at(me * block, block)], load_sem.at[3]),
        pltpu.make_async_copy(index, index_v.at[rep], load_sem.at[4]),
        pltpu.make_async_copy(value, value_v.at[rep], load_sem.at[5]),
        pltpu.make_async_copy(residual, output, load_sem.at[6]),
        pltpu.make_async_copy(right, right_ref, load_sem.at[7]),
        pltpu.make_async_copy(left, left_ref, load_sem.at[8]),
    ]
    for i in (3, 0, 1):
        loads[i].start()

    barrier = pltpu.get_barrier_semaphore()
    has_up, has_dn = z < chips - 1, z > 0

    @pl.when(has_up)
    def _():
        pl.semaphore_signal(barrier, inc=1, device_id={"tp": me + 2}, device_id_type=MESH)

    @pl.when(has_dn)
    def _():
        pl.semaphore_signal(barrier, inc=1, device_id={"tp": me - 2}, device_id_type=MESH)

    pl.semaphore_signal(barrier, inc=1, device_id={"tp": partner}, device_id_type=MESH)
    rounds = replicas.bit_length() - 1
    for turn in range(rounds):
        pl.semaphore_signal(barrier, inc=1, device_id={"rep": flip(rep, 1 << turn)}, device_id_type=MESH)
    pl.semaphore_wait(barrier, 1 + rounds + has_up.astype(jnp.int32) + has_dn.astype(jnp.int32))

    def send(way, s, src, dst):
        return pltpu.make_async_remote_copy(
            src_ref=src, dst_ref=dst, send_sem=step_send.at[way, s], recv_sem=step_recv.at[way, s],
            device_id={"tp": me + (2 if way == 0 else -2)}, device_id_type=MESH,
        )

    def grad_piece(chip, q):
        return dall.at[rows_at((2 * chip + core) * block + q * piece, piece)]

    def to_partner(chip, q):
        return pltpu.make_async_remote_copy(
            src_ref=grad_piece(chip, q), dst_ref=grad_piece(chip, q),
            send_sem=chip_send.at[chip * CHUNKS + q], recv_sem=chip_recv.at[chip * CHUNKS + q],
            device_id={"tp": partner}, device_id_type=MESH,
        )

    lent = units - chips * block

    def hand_over(target):
        return pltpu.make_async_remote_copy(
            src_ref=update.at[pl.ds(lent + target * block, block)],
            dst_ref=weight_grad.at[pl.ds(target * block, block)],
            send_sem=part_send.at[target], recv_sem=part_recv.at[target],
            device_id={"tp": partner}, device_id_type=MESH,
        )

    def comp_copies(turn):
        copies = []
        for m in range(1 << turn):
            holder, spot = flip(rep, m), (1 << turn) - 1 + m
            for kind, (own, all_v) in enumerate(((index, index_v), (value, value_v))):
                copies.append(
                    pltpu.make_async_remote_copy(
                        src_ref=own if m == 0 else all_v.at[holder], dst_ref=all_v.at[holder],
                        send_sem=comp_send.at[kind, spot], recv_sem=comp_recv.at[kind, spot],
                        device_id={"rep": flip(rep, 1 << turn)}, device_id_type=MESH,
                    )
                )
        return copies

    slots = (slot_up, slot_dn)
    rank = (z, chips - 1 - z)
    onward = (has_up, has_dn)
    behind = (has_dn, has_up)

    for q in range(CHUNKS):
        for way in range(2):
            @pl.when(onward[way])
            def _():
                send(way, q, grads.at[pl.ds(q * piece, piece)], grad_piece(z, q)).start()

    for i in (2, 4, 5, 6, 7, 8):
        loads[i].start()
    for copy in comp_copies(0):
        copy.start()

    loads[3].wait()
    for q in range(CHUNKS):
        to_partner(z, q).start()

    def own_sum(target, q):
        return part[rows_at(target * block + q * piece, piece), :]

    def slot_rows(p, q):
        return rows_at((p - 1) * block + q * piece, piece)

    def put_late(source, q):
        return pltpu.make_async_copy(source, late.at[rows_at(q * piece, piece)], late_sem.at[q])

    def service(s):
        p, q = s // CHUNKS, s % CHUNKS
        for way in range(2):
            at, slot = rank[way], slots[way]
            gathered = p < at
            source = z - 1 - p if way == 0 else z + 1 + p
            target = chips + z - 1 - p if way == 0 else z - chips + 1 + p
            summing = jnp.logical_and(jnp.logical_and(p >= at, onward[way]), p < chips - 1)
            first = at == 0

            def pass_on(source):
                after = jnp.logical_and(p == chips - 2, core == way)

                @pl.when(after)
                def _():
                    put_late(source, q).start()

                @pl.when(jnp.logical_not(after))
                def _():
                    send(way, s + CHUNKS, source, slot.at[slot_rows(p + 1, q)]).start()

            @pl.when(jnp.logical_and(behind[way], jnp.logical_or(p < chips - 1, core != way)))
            def _():
                send(way, s, grad_piece(z, q), grad_piece(z, q)).wait_recv()

            @pl.when(gathered)
            def _():
                to_partner(source, q).start()

                @pl.when(onward[way])
                def _():
                    send(way, s + CHUNKS, grad_piece(source, q), grad_piece(source, q)).start()

            @pl.when(jnp.logical_and(summing, first))
            def _():
                pass_on(part.at[rows_at(target * block + q * piece, piece)])

            @pl.when(jnp.logical_and(summing, jnp.logical_not(first)))
            def _():
                here = slot_rows(p, q)
                slot[here, :] = (own_sum(target, q).astype(f32) + slot[here, :].astype(f32)).astype(bf16)
                pass_on(slot.at[here])

    def finish(q):
        here = rows_at(q * piece, piece)
        fin[...] = output[here, :].astype(f32) + own_sum(z, q).astype(f32)
        for way in range(2):
            @pl.when(jnp.logical_and(behind[way], core != way))
            def _():
                fin[...] = fin[...] + slots[way][rows_at((chips - 2) * block + q * piece, piece), :].astype(f32)
        output[here, :] = fin[...].astype(bf16)

    loads[0].wait()
    loads[1].wait()

    def make_hidden(i, carry):
        here = rows_at(i * block, block)
        g = gate_grad[here, :].astype(f32)
        u = up_grad[here, :].astype(f32)
        h = (g * jax.nn.sigmoid(g) * u).astype(bf16)
        hidden[here, :] = h
        hidden_t[:, here] = h.astype(f32).T.astype(bf16)
        return carry

    tile = 512

    def target_at(k):
        return jnp.where(k % 2 == 0, chips - 1 - k // 2, k // 2)

    def add_other(k):
        target = target_at(k)
        hand_over(target).wait_recv()

        def add_part(q, carry):
            here = rows_at(target * block + q * piece, piece)
            part[here, :] = (part[here, :].astype(f32) + weight_grad[here, :].astype(f32)).astype(bf16)
            return carry

        lax.fori_loop(0, CHUNKS, add_part, 0)

    def make_target(k, carry):
        target = target_at(k)
        lax.fori_loop(2 * target, 2 * target + 2, make_hidden, 0)
        rows = rows_at(2 * target * block, 2 * block)
        mine, other = rows_at(target * block, block), rows_at(lent + target * block, block)

        def make_part(i, carry):
            here = rows_at(i * tile, tile)
            got = jnp.dot(hidden[rows, :], w_v[:, here], preferred_element_type=f32).astype(bf16)

            @pl.when(core == 0)
            def _():
                part[mine, here] = got[:block]
                update[other, here] = got[block:]

            @pl.when(core == 1)
            def _():
                part[mine, here] = got[block:]
                update[other, here] = got[:block]
            return carry

        lax.fori_loop(0, model // tile, make_part, 0)
        hand_over(target).start()

        for turn in range(1, rounds):
            @pl.when(k == turn - 1)
            def _():
                for copy in comp_copies(turn - 1):
                    copy.wait_recv()
                for copy in comp_copies(turn):
                    copy.start()

        @pl.when(k > 0)
        def _():
            add_other(k - 1)

        @pl.when(k >= FIRST)
        def _():
            service(k - FIRST)

        return carry

    loads[2].wait()
    lax.fori_loop(0, chips, make_target, 0)

    for copy in comp_copies(rounds - 1):
        copy.wait_recv()
    for i in (4, 5, 7, 8):
        loads[i].wait()

    pairs = replicas // 2
    half = LANES // 2
    spot = lax.broadcasted_iota(jnp.int32, (1, listed), 1)
    lower = spot % LANES < half
    for a in range(span_rows):
        for j in range(pairs):
            for dest, pick in (
                (word_v, lambda r: index_v[r, a]),
                (amount_v, lambda r: value_v[r].astype(f32)[a:a + 1]),
            ):
                even, odd = pick(2 * j), pick(2 * j + 1)
                dest[a, j:j + 1, :] = jnp.where(lower, even, pltpu.roll(odd, half, 1))
                dest[a, pairs + j:pairs + j + 1, :] = jnp.where(lower, pltpu.roll(even, listed - half, 1), odd)

    deep = pairs * LANES
    shift = ((lax.broadcasted_iota(jnp.int32, (replicas, LANES), 1) // TOPK) % 2) * SPAN
    row_place = lax.broadcasted_iota(jnp.int32, (SPAN, deep), 0).astype(f32).astype(bf16)
    col_place = lax.broadcasted_iota(jnp.int32, (2 * SPAN, deep), 0).astype(f32).astype(bf16)

    def decode_row(a):
        def gather(group, carry):
            at = rows_at(group * LANES, LANES)
            words = word_v[a, :, at]
            row_set = (words >> (SPAN.bit_length() - 1)).astype(f32)
            col_set = ((words & (SPAN - 1)) + shift).astype(f32)
            amount_set = amount_v[a, :, at]
            for side in range(2):
                line = lambda x: jnp.concatenate(
                    [x[side * pairs + j:side * pairs + j + 1] for j in range(pairs)], axis=1
                ).astype(bf16)
                row_hot = jnp.where(line(row_set) == row_place, line(amount_set), bf16(0))
                col_hot = jnp.where(line(col_set) == col_place, bf16(1), bf16(0))
                spectral = lax.dot_general(
                    row_hot, col_hot, (((1,), (1,)), ((), ())), preferred_element_type=f32
                )
                mixed[rows_at(group * SPAN, SPAN), side * 2 * SPAN:(side + 1) * 2 * SPAN] = spectral.astype(bf16)
            return carry

        lax.fori_loop(0, groups, gather, 0, unroll=UNROLL)
        halfway = jnp.dot(mixed[...], right_ref[...], preferred_element_type=f32).astype(bf16)
        rows = rows_at(a * SPAN, SPAN)
        for group in range(groups):
            spread = jnp.dot(
                left_ref[...], halfway[group * SPAN:(group + 1) * SPAN], preferred_element_type=f32
            )
            change = (spread * (1.0 / replicas)).astype(bf16)
            at = slice(group * width, (group + 1) * width)
            update[rows, at] = change
            updated[rows, at] = (w_v[rows, at].astype(f32) - learn_rate * change.astype(f32)).astype(bf16)

    def decode_step(a, carry):
        decode_row(a)

        @pl.when(a % 3 == 2)
        def _():
            service(chips - FIRST + a // 3)

        return carry

    add_other(chips - 1)
    for target in range(chips):
        hand_over(target).wait_send()
    lax.fori_loop(0, span_rows, decode_step, 0)
    served = chips - FIRST + span_rows // 3

    low = z < chips // 2

    def grads_of(k, carry):
        chip = jnp.where(low, k, chips - 1 - k)
        for q in range(CHUNKS):
            to_partner(chip, q).wait_recv()
        rows = rows_at(chip * 2 * block, 2 * block)
        back = lax.dot_general(
            dall[rows, :], w_v[...], (((1,), (1,)), ((), ())), preferred_element_type=f32
        )
        g = gate_grad[rows, :].astype(f32)
        u = up_grad[rows, :].astype(f32)
        sig = jax.nn.sigmoid(g)
        gate_grad[rows, :] = (back * u * sig * (1.0 + g * (1.0 - sig))).astype(bf16)
        up_grad[rows, :] = (back * (g * sig)).astype(bf16)
        return carry

    def serve_loop(start, stop):
        lax.fori_loop(start, stop, lambda s, carry: (service(s), carry)[1], 0)

    def grads_early(k, carry):
        grads_of(k, carry)

        @pl.when(served + k < 2 * CHUNKS)
        def _():
            service(served + k)

        return carry

    wide = 256
    turns = model // wide
    last = (chips - 1) * CHUNKS
    near = 2 * block * (chips - 1)
    near_at = jnp.where(low, 0, 2 * block)
    far_at = jnp.where(low, near, 0)
    between = CHUNKS - 1

    def weight_near(i, carry):
        here = rows_at(i * wide, wide)
        rows = pl.ds(pl.multiple_of(near_at, 2 * block), near)
        weight_grad[:, here] = jnp.dot(
            hidden_t[:, rows], dall[rows, here], preferred_element_type=f32
        ).astype(bf16)

        @pl.when(i % (turns // between) == turns // between - 1)
        def _():
            service(2 * CHUNKS + i // (turns // between))

        return carry

    def weight_far(i, carry):
        here = rows_at(i * wide, wide)
        rows = rows_at(far_at, 2 * block)
        more = jnp.dot(hidden_t[:, rows], dall[rows, here], preferred_element_type=f32)
        weight_grad[:, here] = (weight_grad[:, here].astype(f32) + more).astype(bf16)

        @pl.when(i % (turns // CHUNKS) == turns // CHUNKS - 1)
        def _():
            service(last + i // (turns // CHUNKS))
            finish(i // (turns // CHUNKS))

        return carry

    lax.fori_loop(0, chips - 2, grads_early, 0)
    serve_loop(served + chips - 2, 2 * CHUNKS)
    grads_of(chips - 2, 0)
    lax.fori_loop(0, turns, weight_near, 0)
    service(last - 1)
    grads_of(chips - 1, 0)
    loads[6].wait()
    lax.fori_loop(0, turns, weight_far, 0)

    for chip in range(chips):
        for q in range(CHUNKS):
            to_partner(chip, q).wait_send()
    for turn in range(rounds):
        for copy in comp_copies(turn):
            copy.wait_send()
    for way in range(2):
        @pl.when(onward[way])
        def _():
            for s in range(last):
                send(way, s, grad_piece(z, 0), grad_piece(z, 0)).wait_send()

            @pl.when(core != way)
            def _():
                for s in range(last, last + CHUNKS):
                    send(way, s, grad_piece(z, 0), grad_piece(z, 0)).wait_send()

            @pl.when(core == way)
            def _():
                for q in range(CHUNKS):
                    put_late(part.at[pl.ds(0, piece)], q).wait()


def joint_scratch(n, replicas, tokens, units, model, span_rows, listed):
    chips, block = n // 2, tokens // n
    bf16, f32 = jnp.bfloat16, jnp.float32
    dma = pltpu.SemaphoreType.DMA
    arrays = [
        ((tokens, model), bf16),
        (((chips - 1) * block, model), bf16),
        (((chips - 1) * block, model), bf16),
        ((chips * block, model), bf16),
        ((units, model), bf16),
        ((tokens, units), bf16),
        ((units, tokens), bf16),
        ((replicas, span_rows, 1, listed), jnp.int32),
        ((replicas, span_rows, listed), bf16),
        ((span_rows, replicas, listed), jnp.int32),
        ((span_rows, replicas, listed), f32),
        ((listed // LANES * SPAN, LANES // TOPK * SPAN), bf16),
        ((block // CHUNKS, model), f32),
        ((LANES // TOPK * SPAN, LANES // TOPK * SPAN), bf16),
        ((SPAN, SPAN), bf16),
    ]
    total = sum(int(np.prod(shape)) * jnp.dtype(kind).itemsize for shape, kind in arrays)
    steps = chips * CHUNKS
    sems = [
        dma((9,)), dma((2, replicas - 1)), dma((2, replicas - 1)), dma((2, steps)), dma((2, steps)),
        dma((steps,)), dma((steps,)), dma((chips,)), dma((chips,)), dma((CHUNKS,)),
    ]
    return total, [pltpu.VMEM(shape, kind) for shape, kind in arrays] + sems


def joint(residual_r, gate_r, up_r, down_weight, grads_r, index_r, value_r, scratch):
    n, replicas = lax.axis_size("tp"), lax.axis_size("rep")
    (tokens, units), model = gate_r.shape, down_weight.shape[1]
    right, left = decode_tables()
    any_spec = pl.BlockSpec(memory_space=pl.ANY)
    vmem_spec = pl.BlockSpec(memory_space=pltpu.VMEM)
    shapes = [residual_r.shape, (tokens, units), (tokens, units)] + [(units, model)] * 3
    *kept, late = pl.pallas_call(
        functools.partial(joint_kernel, n, replicas),
        out_shape=[pltpu.VMEM(shape, jnp.bfloat16) for shape in shapes]
        + [jax.ShapeDtypeStruct(residual_r.shape, jnp.bfloat16)],
        in_specs=[any_spec] * 9,
        out_specs=[vmem_spec] * 6 + [any_spec],
        scratch_shapes=scratch,
        compiler_params=pltpu.CompilerParams(
            collective_id=0, has_side_effects=True, vmem_limit_bytes=VMEM_BYTES
        ),
        cost_estimate=pl.CostEstimate(
            flops=6 * tokens * units * model, bytes_accessed=units * model * 8, transcendentals=0
        ),
        name="joint",
    )(residual_r, gate_r, up_r, down_weight, grads_r, index_r[:, None], value_r, right, left)
    hops = [(i, i + 2) for i in range(0, n - 2, 2)] + [(i, i - 2) for i in range(3, n, 2)]
    arrived = lax.ppermute(late, "tp", hops)
    early, *kept = kept
    placed = pl.pallas_call(
        put_kernel,
        out_shape=[jax.ShapeDtypeStruct(shape, jnp.bfloat16) for shape in shapes[1:]],
        in_specs=[vmem_spec] * 5,
        out_specs=[any_spec] * 5,
        scratch_shapes=[pltpu.SemaphoreType.DMA((5 * PUT_PARTS,))],
        compiler_params=pltpu.CompilerParams(vmem_limit_bytes=PUT_BYTES),
        cost_estimate=pl.CostEstimate(
            flops=2 * tokens * units * model, bytes_accessed=units * model * 8, transcendentals=0
        ),
        name="put",
    )(*kept)
    output = (early.astype(jnp.float32) + arrived.astype(jnp.float32)).astype(jnp.bfloat16)
    return [output] + list(placed)


def put_kernel(*refs):
    sem = refs[-1]
    count = len(refs) // 2
    copies = []
    for i in range(count):
        rows = refs[i].shape[0] // PUT_PARTS
        for k in range(PUT_PARTS):
            at = pl.ds(k * rows, rows)
            copies.append(
                pltpu.make_async_copy(refs[i].at[at], refs[count + i].at[at], sem.at[i * PUT_PARTS + k])
            )
    for copy in copies:
        copy.start()
    for copy in copies:
        copy.wait()


def chips_rows(n, tokens):
    return n // 2 * (tokens // n)


def shards(residual, gate_pre, up_pre, down_weight, d_out, comp_index, comp_value):
    operands = (residual[0], gate_pre[0], up_pre[0], down_weight, d_out[0], comp_index[0], comp_value[0])
    n, replicas = lax.axis_size("tp"), lax.axis_size("rep")
    tokens, units = gate_pre.shape[1:]
    span_rows, listed = comp_index.shape[1:]
    model = down_weight.shape[1]
    fits = False
    if n % 4 == 0 and units % LANES == 0 and span_rows % 2 == 0 and replicas in (2, 4, 8):
        total, scratch = joint_scratch(n, replicas, tokens, units, model, span_rows, listed)
        fits = total < 36 * 2**20 and units >= chips_rows(n, tokens) and n // 2 == CHUNKS and 2 * CHUNKS >= CHUNKS - FIRST + span_rows // 3 + 2
    if fits:
        outs = joint(*operands, scratch)
    else:
        outs = plain_shards(*operands)
    output, gate_preact_gradient, up_grad, weight_sum, update, updated = outs
    return (
        output[None],
        gate_preact_gradient[None],
        up_grad[None],
        weight_sum[None],
        update,
        updated,
    )


def solution(mesh):
    return jax.shard_map(
        shards,
        mesh=mesh,
        in_specs=(
            P("rep", "tp", None),
            P("rep", None, "tp"),
            P("rep", None, "tp"),
            P("tp", None),
            P("rep", "tp", None),
            P("rep", "tp", None),
            P("rep", "tp", None),
        ),
        out_specs=(
            P("rep", "tp", None),
            P("rep", None, "tp"),
            P("rep", None, "tp"),
            P("rep", "tp", None),
            P("tp", None),
            P("tp", None),
        ),
        check_vma=False,
    )
```

```python
import functools

import jax
import jax.numpy as jnp
import numpy as np
from jax import lax
from jax.experimental import pallas as pl
from jax.experimental.pallas import tpu as pltpu
from jax.sharding import PartitionSpec as P

SPAN = 64
TOPK = 32


learn_rate = 0.02


LANES = 128
UNROLL = 4
MESH = pl.DeviceIdType.MESH
VMEM_BYTES = 38 * 2**20
PUT_BYTES = 2**20
PUT_PARTS = 4
CHUNKS = 4
FIRST = 2


def cosine_table(length):
    freq = np.arange(length, dtype=np.float64)[:, None]
    place = np.arange(length, dtype=np.float64)[None, :]
    scales = np.where(freq == 0, np.sqrt(1.0 / length), np.sqrt(2.0 / length))
    return scales * np.cos(np.pi * (2.0 * place + 1.0) * freq / (2.0 * length))


def decode_kernel(count, *refs):
    index_refs, value_refs = refs[:count], refs[count:2 * count]
    weight_ref, right_ref, left_ref, update_ref, weight_out_ref, mixed_ref = refs[2 * count:]
    groups = index_refs[0].shape[1] // LANES
    per_group = LANES // TOPK
    width = per_group * SPAN
    depth = count * LANES
    lane = lax.broadcasted_iota(jnp.int32, (1, depth), 1)
    shift = ((lane // TOPK) % per_group) * SPAN
    row_place = lax.broadcasted_iota(jnp.int32, (SPAN, depth), 0).astype(jnp.float32).astype(jnp.bfloat16)
    col_place = lax.broadcasted_iota(jnp.int32, (width, depth), 0).astype(jnp.float32).astype(jnp.bfloat16)

    def gather(group, carry):
        at = pl.ds(pl.multiple_of(group * LANES, LANES), LANES)
        words = jnp.concatenate([ref[:, at] for ref in index_refs], axis=1)
        values = jnp.concatenate([ref[:, at] for ref in value_refs], axis=1).astype(jnp.bfloat16)
        rows = (words >> (SPAN.bit_length() - 1)).astype(jnp.float32).astype(jnp.bfloat16)
        cols = ((words & (SPAN - 1)) + shift).astype(jnp.float32).astype(jnp.bfloat16)
        row_hot = jnp.where(rows == row_place, values, jnp.bfloat16(0))
        col_hot = jnp.where(cols == col_place, jnp.bfloat16(1), jnp.bfloat16(0))
        spectral = lax.dot_general(
            row_hot, col_hot, (((1,), (1,)), ((), ())), preferred_element_type=jnp.float32
        )
        mixed_ref[pl.ds(pl.multiple_of(group * SPAN, SPAN), SPAN), :] = spectral.astype(jnp.bfloat16)
        return carry

    lax.fori_loop(0, groups, gather, 0, unroll=UNROLL)
    halfway = jnp.dot(
        mixed_ref[...], right_ref[...], preferred_element_type=jnp.float32
    ).astype(jnp.bfloat16)
    for group in range(groups):
        block = jnp.dot(
            left_ref[...], halfway[group * SPAN:(group + 1) * SPAN], preferred_element_type=jnp.float32
        )
        change = (block * (1.0 / count)).astype(jnp.bfloat16)
        at = slice(group * width, (group + 1) * width)
        update_ref[:, at] = change
        weight_out_ref[:, at] = (
            weight_ref[:, at].astype(jnp.float32) - learn_rate * change.astype(jnp.float32)
        ).astype(jnp.bfloat16)


def decode_tables():
    basis = cosine_table(SPAN)
    right = jnp.asarray(np.kron(np.eye(LANES // TOPK), basis), jnp.bfloat16)
    left = jnp.asarray(basis.T, jnp.bfloat16)
    return right, left


def decode(indices, values, down_weight):
    count = len(indices)
    span_rows, _, listed = indices[0].shape
    units, model = down_weight.shape
    per_group = LANES // TOPK
    width = per_group * SPAN
    right, left = decode_tables()
    strip = pl.BlockSpec((SPAN, model), lambda a: (a, 0))
    whole = lambda shape: pl.BlockSpec(shape, lambda a: (0, 0))
    return pl.pallas_call(
        functools.partial(decode_kernel, count),
        grid=(span_rows,),
        out_shape=[jax.ShapeDtypeStruct((units, model), jnp.bfloat16)] * 2,
        in_specs=[pl.BlockSpec((None, 1, listed), lambda a: (a, 0, 0))] * (2 * count)
        + [strip, whole((width, width)), whole((SPAN, SPAN))],
        out_specs=[strip, strip],
        scratch_shapes=[pltpu.VMEM((listed // LANES * SPAN, width), jnp.bfloat16)],
        compiler_params=pltpu.CompilerParams(
            dimension_semantics=("arbitrary",), vmem_limit_bytes=24 * 2**20
        ),
        cost_estimate=pl.CostEstimate(
            flops=20 * 10**9, bytes_accessed=units * model * 6, transcendentals=0
        ),
        name="decode",
    )(*indices, *values, down_weight, right, left)


def plain_shards(residual_r, gate_r, up_r, down_weight, grads_r, index_r, value_r):
    replicas = lax.axis_size("rep")

    def from_replicas(mine):
        return [mine] + [
            lax.ppermute(mine, "rep", [(i, (i + step) % replicas) for i in range(replicas)])
            for step in range(1, replicas)
        ]

    indices = from_replicas(index_r[:, None])
    values = from_replicas(value_r.astype(jnp.float32)[:, None])
    gate_f = gate_r.astype(jnp.float32)
    up_f = up_r.astype(jnp.float32)
    sigmoid_g = jax.nn.sigmoid(gate_f)
    activated = gate_f * sigmoid_g
    hidden = (activated * up_f).astype(jnp.bfloat16)
    summed = lax.psum_scatter(
        jnp.dot(hidden, down_weight, preferred_element_type=jnp.float32).astype(jnp.bfloat16),
        "tp",
        scatter_dimension=0,
        tiled=True,
    ).astype(jnp.float32)
    incoming = lax.all_gather(grads_r, "tp", axis=0, tiled=True)
    hidden_grad = lax.dot_general(
        incoming, down_weight, (((1,), (1,)), ((), ())), preferred_element_type=jnp.float32
    )
    weight_sum = lax.dot_general(
        hidden, incoming, (((0,), (0,)), ((), ())), preferred_element_type=jnp.float32
    )
    output = (residual_r.astype(jnp.float32) + summed).astype(jnp.bfloat16)
    gate_preact_gradient = (
        hidden_grad * up_f * sigmoid_g * (1.0 + gate_f * (1.0 - sigmoid_g))
    ).astype(jnp.bfloat16)
    up_grad = (hidden_grad * activated).astype(jnp.bfloat16)
    update, updated_down_weight = decode(indices, values, down_weight)
    return output, gate_preact_gradient, up_grad, weight_sum.astype(jnp.bfloat16), update, updated_down_weight


def rows_at(start, size):
    return pl.ds(pl.multiple_of(start, size), size)


def flip(place, bits):
    for k in range(bits.bit_length()):
        if (bits >> k) & 1:
            place = place + (1 << k) * (1 - 2 * ((place // (1 << k)) % 2))
    return place


def joint_kernel(
    n, replicas,
    residual, gate, up, weight, grads, index, value, right, left,
    output, gate_grad, up_grad, weight_grad, update, updated, late,
    dall, slot_up, slot_dn, part, w_v, hidden, hidden_t,
    index_v, value_v, word_v, amount_v, mixed, fin, right_ref, left_ref,
    load_sem, comp_send, comp_recv, step_send, step_recv, chip_send, chip_recv,
    part_send, part_recv, late_sem,
):
    chips = n // 2
    rep = lax.axis_index("rep")
    me = lax.axis_index("tp")
    z, core = me // 2, me % 2
    partner = me + 1 - 2 * core
    tokens, units = gate_grad.shape
    model = w_v.shape[1]
    block = tokens // n
    piece = block // CHUNKS
    span_rows, listed = value_v.shape[1], value_v.shape[2]
    groups = listed // LANES
    per_group = LANES // TOPK
    width = per_group * SPAN
    f32, bf16 = jnp.float32, jnp.bfloat16

    loads = [
        pltpu.make_async_copy(gate, gate_grad, load_sem.at[0]),
        pltpu.make_async_copy(up, up_grad, load_sem.at[1]),
        pltpu.make_async_copy(weight, w_v, load_sem.at[2]),
        pltpu.make_async_copy(grads, dall.at[rows_at(me * block, block)], load_sem.at[3]),
        pltpu.make_async_copy(index, index_v.at[rep], load_sem.at[4]),
        pltpu.make_async_copy(value, value_v.at[rep], load_sem.at[5]),
        pltpu.make_async_copy(residual, output, load_sem.at[6]),
        pltpu.make_async_copy(right, right_ref, load_sem.at[7]),
        pltpu.make_async_copy(left, left_ref, load_sem.at[8]),
    ]
    loads[3].start()

    barrier = pltpu.get_barrier_semaphore()
    has_up, has_dn = z < chips - 1, z > 0

    @pl.when(has_up)
    def _():
        pl.semaphore_signal(barrier, inc=1, device_id={"tp": me + 2}, device_id_type=MESH)

    @pl.when(has_dn)
    def _():
        pl.semaphore_signal(barrier, inc=1, device_id={"tp": me - 2}, device_id_type=MESH)

    pl.semaphore_signal(barrier, inc=1, device_id={"tp": partner}, device_id_type=MESH)
    rounds = replicas.bit_length() - 1
    for turn in range(rounds):
        pl.semaphore_signal(barrier, inc=1, device_id={"rep": flip(rep, 1 << turn)}, device_id_type=MESH)
    loads[0].start()
    loads[1].start()
    loads[3].wait()
    pl.semaphore_wait(barrier, 1 + rounds + has_up.astype(jnp.int32) + has_dn.astype(jnp.int32))

    def send(way, s, src, dst):
        return pltpu.make_async_remote_copy(
            src_ref=src, dst_ref=dst, send_sem=step_send.at[way, s], recv_sem=step_recv.at[way, s],
            device_id={"tp": me + (2 if way == 0 else -2)}, device_id_type=MESH,
        )

    def grad_piece(chip, q):
        return dall.at[rows_at((2 * chip + core) * block + q * piece, piece)]

    def to_partner(chip, q):
        return pltpu.make_async_remote_copy(
            src_ref=grad_piece(chip, q), dst_ref=grad_piece(chip, q),
            send_sem=chip_send.at[chip * CHUNKS + q], recv_sem=chip_recv.at[chip * CHUNKS + q],
            device_id={"tp": partner}, device_id_type=MESH,
        )

    lent = units - chips * block

    def hand_over(target):
        return pltpu.make_async_remote_copy(
            src_ref=update.at[pl.ds(lent + target * block, block)],
            dst_ref=weight_grad.at[pl.ds(target * block, block)],
            send_sem=part_send.at[target], recv_sem=part_recv.at[target],
            device_id={"tp": partner}, device_id_type=MESH,
        )

    def comp_copies(turn):
        copies = []
        for m in range(1 << turn):
            holder, spot = flip(rep, m), (1 << turn) - 1 + m
            for kind, (own, all_v) in enumerate(((index, index_v), (value, value_v))):
                copies.append(
                    pltpu.make_async_remote_copy(
                        src_ref=own if m == 0 else all_v.at[holder], dst_ref=all_v.at[holder],
                        send_sem=comp_send.at[kind, spot], recv_sem=comp_recv.at[kind, spot],
                        device_id={"rep": flip(rep, 1 << turn)}, device_id_type=MESH,
                    )
                )
        return copies

    slots = (slot_up, slot_dn)
    rank = (z, chips - 1 - z)
    onward = (has_up, has_dn)
    behind = (has_dn, has_up)

    for q in range(CHUNKS):
        for way in range(2):
            @pl.when(onward[way])
            def _():
                send(way, q, grad_piece(z, q), grad_piece(z, q)).start()

    for i in (2, 4, 5, 6, 7, 8):
        loads[i].start()
    for copy in comp_copies(0):
        copy.start()

    for q in range(CHUNKS):
        to_partner(z, q).start()

    def own_sum(target, q):
        return part[rows_at(target * block + q * piece, piece), :]

    def slot_rows(p, q):
        return rows_at((p - 1) * block + q * piece, piece)

    def put_late(source, q):
        return pltpu.make_async_copy(source, late.at[rows_at(q * piece, piece)], late_sem.at[q])

    def service(s):
        p, q = s // CHUNKS, s % CHUNKS
        for way in range(2):
            at, slot = rank[way], slots[way]
            gathered = p < at
            source = z - 1 - p if way == 0 else z + 1 + p
            target = chips + z - 1 - p if way == 0 else z - chips + 1 + p
            summing = jnp.logical_and(jnp.logical_and(p >= at, onward[way]), p < chips - 1)
            first = at == 0

            def pass_on(source):
                after = jnp.logical_and(p == chips - 2, core == way)

                @pl.when(after)
                def _():
                    put_late(source, q).start()

                @pl.when(jnp.logical_not(after))
                def _():
                    send(way, s + CHUNKS, source, slot.at[slot_rows(p + 1, q)]).start()

            @pl.when(jnp.logical_and(behind[way], jnp.logical_or(p < chips - 1, core != way)))
            def _():
                send(way, s, grad_piece(z, q), grad_piece(z, q)).wait_recv()

            @pl.when(gathered)
            def _():
                to_partner(source, q).start()

                @pl.when(onward[way])
                def _():
                    send(way, s + CHUNKS, grad_piece(source, q), grad_piece(source, q)).start()

            @pl.when(jnp.logical_and(summing, first))
            def _():
                pass_on(part.at[rows_at(target * block + q * piece, piece)])

            @pl.when(jnp.logical_and(summing, jnp.logical_not(first)))
            def _():
                here = slot_rows(p, q)
                slot[here, :] = (own_sum(target, q).astype(f32) + slot[here, :].astype(f32)).astype(bf16)
                pass_on(slot.at[here])

    def finish(q):
        here = rows_at(q * piece, piece)
        fin[...] = output[here, :].astype(f32) + own_sum(z, q).astype(f32)
        for way in range(2):
            @pl.when(jnp.logical_and(behind[way], core != way))
            def _():
                fin[...] = fin[...] + slots[way][rows_at((chips - 2) * block + q * piece, piece), :].astype(f32)
        output[here, :] = fin[...].astype(bf16)

    loads[0].wait()
    loads[1].wait()

    def make_hidden(i, carry):
        here = rows_at(i * block, block)
        g = gate_grad[here, :].astype(f32)
        u = up_grad[here, :].astype(f32)
        h = (g * jax.nn.sigmoid(g) * u).astype(bf16)
        hidden[here, :] = h
        hidden_t[:, here] = h.astype(f32).T.astype(bf16)
        return carry

    tile = 512

    def target_at(k):
        return jnp.where(k % 2 == 0, chips - 1 - k // 2, k // 2)

    def add_other(k):
        target = target_at(k)
        hand_over(target).wait_recv()

        def add_part(q, carry):
            here = rows_at(target * block + q * piece, piece)
            part[here, :] = (part[here, :].astype(f32) + weight_grad[here, :].astype(f32)).astype(bf16)
            return carry

        lax.fori_loop(0, CHUNKS, add_part, 0)

    def make_target(k, carry):
        target = target_at(k)
        lax.fori_loop(2 * target, 2 * target + 2, make_hidden, 0)
        rows = rows_at(2 * target * block, 2 * block)
        mine, other = rows_at(target * block, block), rows_at(lent + target * block, block)

        def make_part(i, carry):
            here = rows_at(i * tile, tile)
            got = jnp.dot(hidden[rows, :], w_v[:, here], preferred_element_type=f32).astype(bf16)

            @pl.when(core == 0)
            def _():
                part[mine, here] = got[:block]
                update[other, here] = got[block:]

            @pl.when(core == 1)
            def _():
                part[mine, here] = got[block:]
                update[other, here] = got[:block]
            return carry

        lax.fori_loop(0, model // tile, make_part, 0)
        hand_over(target).start()

        for turn in range(1, rounds):
            @pl.when(k == turn - 1)
            def _():
                for copy in comp_copies(turn - 1):
                    copy.wait_recv()
                for copy in comp_copies(turn):
                    copy.start()

        @pl.when(k > 0)
        def _():
            add_other(k - 1)

        @pl.when(k >= FIRST)
        def _():
            service(k - FIRST)

        return carry

    loads[2].wait()
    lax.fori_loop(0, chips, make_target, 0)

    for copy in comp_copies(rounds - 1):
        copy.wait_recv()
    for i in (4, 5, 7, 8):
        loads[i].wait()

    pairs = replicas // 2
    half = LANES // 2
    spot = lax.broadcasted_iota(jnp.int32, (1, listed), 1)
    lower = spot % LANES < half
    for a in range(span_rows):
        for j in range(pairs):
            for dest, pick in (
                (word_v, lambda r: index_v[r, a]),
                (amount_v, lambda r: value_v[r].astype(f32)[a:a + 1]),
            ):
                even, odd = pick(2 * j), pick(2 * j + 1)
                dest[a, j:j + 1, :] = jnp.where(lower, even, pltpu.roll(odd, half, 1))
                dest[a, pairs + j:pairs + j + 1, :] = jnp.where(lower, pltpu.roll(even, listed - half, 1), odd)

    deep = pairs * LANES
    shift = ((lax.broadcasted_iota(jnp.int32, (replicas, LANES), 1) // TOPK) % 2) * SPAN
    row_place = lax.broadcasted_iota(jnp.int32, (SPAN, deep), 0).astype(f32).astype(bf16)
    col_place = lax.broadcasted_iota(jnp.int32, (2 * SPAN, deep), 0).astype(f32).astype(bf16)

    def decode_row(a):
        def gather(group, carry):
            at = rows_at(group * LANES, LANES)
            words = word_v[a, :, at]
            row_set = (words >> (SPAN.bit_length() - 1)).astype(f32)
            col_set = ((words & (SPAN - 1)) + shift).astype(f32)
            amount_set = amount_v[a, :, at]
            for side in range(2):
                line = lambda x: jnp.concatenate(
                    [x[side * pairs + j:side * pairs + j + 1] for j in range(pairs)], axis=1
                ).astype(bf16)
                row_hot = jnp.where(line(row_set) == row_place, line(amount_set), bf16(0))
                col_hot = jnp.where(line(col_set) == col_place, bf16(1), bf16(0))
                spectral = lax.dot_general(
                    row_hot, col_hot, (((1,), (1,)), ((), ())), preferred_element_type=f32
                )
                mixed[rows_at(group * SPAN, SPAN), side * 2 * SPAN:(side + 1) * 2 * SPAN] = spectral.astype(bf16)
            return carry

        lax.fori_loop(0, groups, gather, 0, unroll=UNROLL)
        halfway = jnp.dot(mixed[...], right_ref[...], preferred_element_type=f32).astype(bf16)
        rows = rows_at(a * SPAN, SPAN)
        for group in range(groups):
            spread = jnp.dot(
                left_ref[...], halfway[group * SPAN:(group + 1) * SPAN], preferred_element_type=f32
            )
            change = (spread * (1.0 / replicas)).astype(bf16)
            at = slice(group * width, (group + 1) * width)
            update[rows, at] = change
            updated[rows, at] = (w_v[rows, at].astype(f32) - learn_rate * change.astype(f32)).astype(bf16)

    def decode_step(a, carry):
        decode_row(a)

        @pl.when(a % 3 == 2)
        def _():
            service(chips - FIRST + a // 3)

        return carry

    add_other(chips - 1)
    for target in range(chips):
        hand_over(target).wait_send()
    lax.fori_loop(0, span_rows, decode_step, 0)
    served = chips - FIRST + span_rows // 3

    low = z < chips // 2

    def grads_of(k, carry):
        chip = jnp.where(low, k, chips - 1 - k)
        for q in range(CHUNKS):
            to_partner(chip, q).wait_recv()
        rows = rows_at(chip * 2 * block, 2 * block)
        back = lax.dot_general(
            dall[rows, :], w_v[...], (((1,), (1,)), ((), ())), preferred_element_type=f32
        )
        g = gate_grad[rows, :].astype(f32)
        u = up_grad[rows, :].astype(f32)
        sig = jax.nn.sigmoid(g)
        gate_grad[rows, :] = (back * u * sig * (1.0 + g * (1.0 - sig))).astype(bf16)
        up_grad[rows, :] = (back * (g * sig)).astype(bf16)
        return carry

    def serve_loop(start, stop):
        lax.fori_loop(start, stop, lambda s, carry: (service(s), carry)[1], 0)

    def grads_early(k, carry):
        grads_of(k, carry)

        @pl.when(served + k < 2 * CHUNKS)
        def _():
            service(served + k)

        return carry

    wide = 256
    turns = model // wide
    last = (chips - 1) * CHUNKS
    near = 2 * block * (chips - 1)
    near_at = jnp.where(low, 0, 2 * block)
    far_at = jnp.where(low, near, 0)
    between = CHUNKS - 1

    def weight_near(i, carry):
        here = rows_at(i * wide, wide)
        rows = pl.ds(pl.multiple_of(near_at, 2 * block), near)
        weight_grad[:, here] = jnp.dot(
            hidden_t[:, rows], dall[rows, here], preferred_element_type=f32
        ).astype(bf16)

        @pl.when(i % (turns // between) == turns // between - 1)
        def _():
            service(2 * CHUNKS + i // (turns // between))

        return carry

    def weight_far(i, carry):
        here = rows_at(i * wide, wide)
        rows = rows_at(far_at, 2 * block)
        more = jnp.dot(hidden_t[:, rows], dall[rows, here], preferred_element_type=f32)
        weight_grad[:, here] = (weight_grad[:, here].astype(f32) + more).astype(bf16)

        @pl.when(i % (turns // CHUNKS) == turns // CHUNKS - 1)
        def _():
            service(last + i // (turns // CHUNKS))
            finish(i // (turns // CHUNKS))

        return carry

    lax.fori_loop(0, chips - 2, grads_early, 0)
    serve_loop(served + chips - 2, 2 * CHUNKS)
    grads_of(chips - 2, 0)
    lax.fori_loop(0, turns, weight_near, 0)
    service(last - 1)
    grads_of(chips - 1, 0)
    loads[6].wait()
    lax.fori_loop(0, turns, weight_far, 0)

    for chip in range(chips):
        for q in range(CHUNKS):
            to_partner(chip, q).wait_send()
    for turn in range(rounds):
        for copy in comp_copies(turn):
            copy.wait_send()
    for way in range(2):
        @pl.when(onward[way])
        def _():
            for s in range(last):
                send(way, s, grad_piece(z, 0), grad_piece(z, 0)).wait_send()

            @pl.when(core != way)
            def _():
                for s in range(last, last + CHUNKS):
                    send(way, s, grad_piece(z, 0), grad_piece(z, 0)).wait_send()

            @pl.when(core == way)
            def _():
                for q in range(CHUNKS):
                    put_late(part.at[pl.ds(0, piece)], q).wait()


def joint_scratch(n, replicas, tokens, units, model, span_rows, listed):
    chips, block = n // 2, tokens // n
    bf16, f32 = jnp.bfloat16, jnp.float32
    dma = pltpu.SemaphoreType.DMA
    arrays = [
        ((tokens, model), bf16),
        (((chips - 1) * block, model), bf16),
        (((chips - 1) * block, model), bf16),
        ((chips * block, model), bf16),
        ((units, model), bf16),
        ((tokens, units), bf16),
        ((units, tokens), bf16),
        ((replicas, span_rows, 1, listed), jnp.int32),
        ((replicas, span_rows, listed), bf16),
        ((span_rows, replicas, listed), jnp.int32),
        ((span_rows, replicas, listed), f32),
        ((listed // LANES * SPAN, LANES // TOPK * SPAN), bf16),
        ((block // CHUNKS, model), f32),
        ((LANES // TOPK * SPAN, LANES // TOPK * SPAN), bf16),
        ((SPAN, SPAN), bf16),
    ]
    total = sum(int(np.prod(shape)) * jnp.dtype(kind).itemsize for shape, kind in arrays)
    steps = chips * CHUNKS
    sems = [
        dma((9,)), dma((2, replicas - 1)), dma((2, replicas - 1)), dma((2, steps)), dma((2, steps)),
        dma((steps,)), dma((steps,)), dma((chips,)), dma((chips,)), dma((CHUNKS,)),
    ]
    return total, [pltpu.VMEM(shape, kind) for shape, kind in arrays] + sems


def joint(residual_r, gate_r, up_r, down_weight, grads_r, index_r, value_r, scratch):
    n, replicas = lax.axis_size("tp"), lax.axis_size("rep")
    (tokens, units), model = gate_r.shape, down_weight.shape[1]
    right, left = decode_tables()
    any_spec = pl.BlockSpec(memory_space=pl.ANY)
    vmem_spec = pl.BlockSpec(memory_space=pltpu.VMEM)
    shapes = [residual_r.shape, (tokens, units), (tokens, units)] + [(units, model)] * 3
    *kept, late = pl.pallas_call(
        functools.partial(joint_kernel, n, replicas),
        out_shape=[pltpu.VMEM(shape, jnp.bfloat16) for shape in shapes]
        + [jax.ShapeDtypeStruct(residual_r.shape, jnp.bfloat16)],
        in_specs=[any_spec] * 9,
        out_specs=[vmem_spec] * 6 + [any_spec],
        scratch_shapes=scratch,
        compiler_params=pltpu.CompilerParams(
            collective_id=0, has_side_effects=True, vmem_limit_bytes=VMEM_BYTES
        ),
        cost_estimate=pl.CostEstimate(
            flops=6 * tokens * units * model, bytes_accessed=units * model * 8, transcendentals=0
        ),
        name="joint",
    )(residual_r, gate_r, up_r, down_weight, grads_r, index_r[:, None], value_r, right, left)
    hops = [(i, i + 2) for i in range(0, n - 2, 2)] + [(i, i - 2) for i in range(3, n, 2)]
    arrived = lax.ppermute(late, "tp", hops)
    early, *kept = kept
    placed = pl.pallas_call(
        put_kernel,
        out_shape=[jax.ShapeDtypeStruct(shape, jnp.bfloat16) for shape in shapes[1:]],
        in_specs=[vmem_spec] * 5,
        out_specs=[any_spec] * 5,
        scratch_shapes=[pltpu.SemaphoreType.DMA((5 * PUT_PARTS,))],
        compiler_params=pltpu.CompilerParams(vmem_limit_bytes=PUT_BYTES),
        cost_estimate=pl.CostEstimate(
            flops=2 * tokens * units * model, bytes_accessed=units * model * 8, transcendentals=0
        ),
        name="put",
    )(*kept)
    output = (early.astype(jnp.float32) + arrived.astype(jnp.float32)).astype(jnp.bfloat16)
    return [output] + list(placed)


def put_kernel(*refs):
    sem = refs[-1]
    count = len(refs) // 2
    copies = []
    for i in range(count):
        rows = refs[i].shape[0] // PUT_PARTS
        for k in range(PUT_PARTS):
            at = pl.ds(k * rows, rows)
            copies.append(
                pltpu.make_async_copy(refs[i].at[at], refs[count + i].at[at], sem.at[i * PUT_PARTS + k])
            )
    for copy in copies:
        copy.start()
    for copy in copies:
        copy.wait()


def chips_rows(n, tokens):
    return n // 2 * (tokens // n)


def shards(residual, gate_pre, up_pre, down_weight, d_out, comp_index, comp_value):
    operands = (residual[0], gate_pre[0], up_pre[0], down_weight, d_out[0], comp_index[0], comp_value[0])
    n, replicas = lax.axis_size("tp"), lax.axis_size("rep")
    tokens, units = gate_pre.shape[1:]
    span_rows, listed = comp_index.shape[1:]
    model = down_weight.shape[1]
    fits = False
    if n % 4 == 0 and units % LANES == 0 and span_rows % 2 == 0 and replicas in (2, 4, 8):
        total, scratch = joint_scratch(n, replicas, tokens, units, model, span_rows, listed)
        fits = total < 36 * 2**20 and units >= chips_rows(n, tokens) and n // 2 == CHUNKS and 2 * CHUNKS >= CHUNKS - FIRST + span_rows // 3 + 2
    if fits:
        outs = joint(*operands, scratch)
    else:
        outs = plain_shards(*operands)
    output, gate_preact_gradient, up_grad, weight_sum, update, updated = outs
    return (
        output[None],
        gate_preact_gradient[None],
        up_grad[None],
        weight_sum[None],
        update,
        updated,
    )


def solution(mesh):
    return jax.shard_map(
        shards,
        mesh=mesh,
        in_specs=(
            P("rep", "tp", None),
            P("rep", None, "tp"),
            P("rep", None, "tp"),
            P("tp", None),
            P("rep", "tp", None),
            P("rep", "tp", None),
            P("rep", "tp", None),
        ),
        out_specs=(
            P("rep", "tp", None),
            P("rep", None, "tp"),
            P("rep", None, "tp"),
            P("rep", "tp", None),
            P("tp", None),
            P("tp", None),
        ),
        check_vma=False,
    )
```
